16 devices in a mesh: dp: 2 (over y, z), dcp: 8 (over x, core).
Axes of the slice: x: 4, y: 2, z: 1, core: 2. Of those that a mesh axis runs over, the one named last changes fastest.
The devices are a block of a 4x4x8 slice.
Arguments:
- q_abs: bfloat16 [128, 2, 128, 576], P('dp', None, 'dcp'), parts along dimension 0
- kv_cache: bfloat16 [128, 16, 8, 64, 576], P('dp', None, 'dcp'), parts along dimension 0
- lengths: int32 [128], P('dp'), parts along dimension 0
Outputs:
- output: bfloat16 [128, 2, 128, 512], P('dp', None, 'dcp'), parts along dimension 0
There are 2 independent parts. The reference program is written for one: setup_inputs(seed, part) draws one part's arguments, and reference() takes and returns one part's arrays. A program takes and returns all parts, laid end to end along the dimension named above; each array names one.
All inputs are finite; a program needn't handle non-finite values.
Results may differ from the reference program's by a relative error of at most 0.00759048.
Values are sent between devices in bfloat16 or wider.
A program may use at most 768 MiB of HBM per device.

```python
import math
import jax
import jax.numpy as jnp
from jax import lax

BATCH = 64
MTP = 2
HEADS = 128
LATENT = 512
ROPE = 64
NOPE = 128
ROUNDS = 16
GROUP = 8
PAGE = 64

SEQ = ROUNDS * GROUP * PAGE
WIDTH = LATENT + ROPE


def setup_inputs(seed: int = 0, part: int = 0) -> dict:
    base_key = jax.random.fold_in(jax.random.key(seed), part)
    key_qlat, key_qrope, key_cache, key_len, key_pick = jax.random.split(base_key, 5)
    lat_scale = math.sqrt(SEQ / 256.0)
    q_lat = jax.random.normal(key_qlat, (BATCH, MTP, HEADS, LATENT), jnp.float32) * (math.sqrt(1.8 * (NOPE + ROPE) / LATENT) / lat_scale)
    q_rope = jax.random.normal(key_qrope, (BATCH, MTP, HEADS, ROPE), jnp.float32) * math.sqrt(1.8 * (NOPE + ROPE) / ROPE)
    q_abs = jnp.concatenate([q_lat, q_rope], axis=-1).astype(jnp.bfloat16)
    col_scale = jnp.where(jnp.arange(WIDTH) < LATENT, lat_scale, 1.0)
    kv_cache = (jax.random.normal(key_cache, (BATCH, ROUNDS, GROUP, PAGE, WIDTH), jnp.float32) * col_scale).astype(jnp.bfloat16)
    lengths = jax.random.randint(key_len, (BATCH,), SEQ // 2, SEQ + 1, dtype=jnp.int32)
    longest = jax.random.randint(key_pick, (), 0, BATCH, dtype=jnp.int32)
    lengths = jnp.where(jnp.arange(BATCH) == longest, SEQ, lengths).astype(jnp.int32)
    return {'q_abs': q_abs, 'kv_cache': kv_cache, 'lengths': lengths}


def reference(q_abs, kv_cache, lengths):
    keys_all = kv_cache.reshape(BATCH, SEQ, WIDTH)
    score_scale = (NOPE + ROPE) ** -0.5
    positions = jnp.arange(SEQ)
    offsets = jnp.arange(MTP) - MTP

    def one_seq(seq_args):
        q_seq, key_seq, length = seq_args
        key_f = key_seq.astype(jnp.float32)
        scores = jnp.einsum('thd,sd->ths', q_seq.astype(jnp.float32), key_f) * score_scale
        last_pos = length + offsets
        visible = positions[None, :] <= last_pos[:, None]
        scores = jnp.where(visible[:, None, :], scores, -jnp.inf)
        weights = jax.nn.softmax(scores, axis=-1)
        out_seq = jnp.einsum('ths,sc->thc', weights, key_f[:, :LATENT])
        return out_seq.astype(jnp.bfloat16)

    return lax.map(one_seq, (q_abs, keys_all, lengths))
```

```python
import functools
import math

import jax
import jax.numpy as jnp
from jax import lax
from jax.experimental import pallas as pl
from jax.experimental.pallas import tpu as pltpu
from jax.sharding import PartitionSpec as P

LATENT = 512
ROPE = 64
NOPE = 128
PAGE = 64
CORES = 2
SCALE2 = (NOPE + ROPE) ** -0.5 * math.log2(math.e)

GQ = 4
GO = 8
KV_SLOTS = 4
AHEAD = 3
HOLD = 13


def _kernel(sizes, q_hbm, kv_hbm, len_ref, out_hbm,
            qall, rope_in, kvb, o_all, prx, abuf, bbuf,
            lse_all, plse, clse, alse, nlse, blse, wt,
            load_sem, kv_sem, out_sem, qs, qr, ds, dr, as_, ar, bs, br):
    batch, toks, heads, npos, group = sizes
    chips = group // CORES
    rows = toks * heads
    half = GO // 2
    n_q, n_o = batch // GQ, batch // GO
    me = lax.axis_index('dcp')
    c, k = me // CORES, me % CORES
    ok = 1 - k
    cr, cl, cf = (c + 1) % chips, (c + chips - 1) % chips, (c + 2) % chips
    right, left, partner = cr * CORES + k, cl * CORES + k, c * CORES + ok

    barrier = pltpu.get_barrier_semaphore()
    for other in (right, left, partner):
        pl.semaphore_signal(barrier, inc=1, device_id={'dcp': other}, device_id_type=pl.DeviceIdType.MESH)

    def rcopy(src, dst, send, recv, dev):
        return pltpu.make_async_remote_copy(src_ref=src, dst_ref=dst, send_sem=send, recv_sem=recv,
                                            device_id={'dcp': dev}, device_id_type=pl.DeviceIdType.MESH)

    loads = [pltpu.make_async_copy(q_hbm.at[:, t, :, 0:LATENT], qall.at[k, c, :, :, t * LATENT:(t + 1) * LATENT], load_sem.at[t])
             for t in range(toks)]
    loads.append(pltpu.make_async_copy(q_hbm.at[:, :, :, LATENT:LATENT + ROPE], rope_in, load_sem.at[toks]))
    for cp in loads:
        cp.start()

    def kv_copy(b):
        slot = lax.rem(b, KV_SLOTS)
        return pltpu.make_async_copy(kv_hbm.at[b], kvb.at[slot], kv_sem.at[slot])

    for b in range(KV_SLOTS):
        kv_copy(b).start()
    loads[toks].wait()

    def pack(b, carry):
        both = [rope_in[b, t] for t in range(toks)]
        qall[k, c, b, :, toks * LATENT:] = jnp.concatenate(both, axis=-1)
        return carry

    lax.fori_loop(0, batch, pack, 0)
    for t in range(toks):
        loads[t].wait()
    pl.semaphore_wait(barrier, 3)

    def qreg(kk, cc, b0, n):
        return qall.at[kk, cc, pl.ds(b0, n)]

    def q_own(j):
        r = qreg(k, c, j * GQ, GQ)
        return [rcopy(r, r, qs.at[0, j], qr.at[0, j], right), rcopy(r, r, qs.at[1, j], qr.at[1, j], left),
                rcopy(r, r, qs.at[2, j], qr.at[2, j], partner)]

    def q_relay(j):
        lr, rr = qreg(k, cl, j * GQ, GQ), qreg(k, cr, j * GQ, GQ)
        lh, rh = qreg(k, cl, j * GQ, GQ // 2), qreg(k, cr, j * GQ + GQ // 2, GQ // 2)
        return [rcopy(lh, lh, qs.at[3, j], qr.at[3, j], right), rcopy(rh, rh, qs.at[4, j], qr.at[4, j], left),
                rcopy(lr, lr, qs.at[5, j], qr.at[5, j], partner), rcopy(rr, rr, qs.at[6, j], qr.at[6, j], partner)]

    def q_far(j):
        f0, f1 = qreg(k, cf, j * GQ, GQ // 2), qreg(k, cf, j * GQ + GQ // 2, GQ // 2)
        return [rcopy(f0, f0, qs.at[7, j], qr.at[7, j], partner), rcopy(f1, f1, qs.at[8, j], qr.at[8, j], partner)]

    def q_arrival(kind, j):
        full, h0, h1 = (j * GQ, GQ), (j * GQ, GQ // 2), (j * GQ + GQ // 2, GQ // 2)
        kk, cc, span = [(k, cl, full), (k, cr, full), (ok, c, full), (k, cf, h0), (k, cf, h1),
                        (ok, cl, full), (ok, cr, full), (ok, cf, h0), (ok, cf, h1)][kind]
        r = qreg(kk, cc, *span)
        return rcopy(r, r, qs.at[kind, j], qr.at[kind, j], partner)

    row_tok = (lax.broadcasted_iota(jnp.int32, (CORES * chips * rows, 1), 0) // heads) % toks
    key = lax.broadcasted_iota(jnp.int32, (1, npos), 1)
    pos = ((key // PAGE) * group + me) * PAGE + key % PAGE
    lanes = chips * rows
    eye = lax.broadcasted_iota(jnp.int32, (lanes, lanes), 0) == lax.broadcasted_iota(jnp.int32, (lanes, lanes), 1)

    def attend(b):
        kv_copy(b).wait()
        slot = lax.rem(b, KV_SLOTS)
        q = qall[:, :, b].reshape(CORES * chips, heads, toks * (LATENT + ROPE))
        lat = jnp.stack([q[:, :, t * LATENT:(t + 1) * LATENT] for t in range(toks)], axis=1).reshape(-1, LATENT)
        rope0 = toks * LATENT
        rope = jnp.stack([q[:, :, rope0 + t * ROPE:rope0 + (t + 1) * ROPE] for t in range(toks)], axis=1).reshape(-1, ROPE)
        q_rows = jnp.concatenate([lat, rope], axis=-1)
        s = lax.dot_general(q_rows, kvb[slot], (((1,), (1,)), ((), ())), preferred_element_type=jnp.float32)
        s = jnp.where(pos <= len_ref[b] - toks + row_tok, s, -jnp.inf)
        m = jnp.max(s, axis=-1, keepdims=True)
        p = jnp.exp2((s - m) * SCALE2)
        l = jnp.sum(p, axis=-1, keepdims=True)
        o = jnp.dot(p.astype(jnp.bfloat16), kvb[slot, :, 0:LATENT], preferred_element_type=jnp.float32)
        o = (o * (1.0 / l)).astype(jnp.bfloat16)
        o_all[:, :, b] = o.reshape(CORES, chips, rows, LATENT)
        lse = m * SCALE2 + jnp.log2(l)
        for kk in range(CORES):
            col = lse[kk * lanes:(kk + 1) * lanes]
            lse_all[kk, pl.ds(b, 1)] = jnp.sum(jnp.where(eye, col, 0.0), axis=0, keepdims=True)

        @pl.when(b + KV_SLOTS < batch)
        def _():
            kv_copy(b + KV_SLOTS).start()

    def seqs(i, n=GO):
        return pl.ds(pl.multiple_of(i * n, n), n)

    def d_send(i):
        return [rcopy(o_all.at[ok, :, seqs(i)], prx.at[:, seqs(i)], ds.at[0, i], dr.at[0, i], partner),
                rcopy(lse_all.at[ok, seqs(i)], plse.at[seqs(i)], ds.at[1, i], dr.at[1, i], partner)]

    def d_merge(i):
        for cp in d_send(i):
            cp.wait_recv()
        a, b = lse_all[k, seqs(i)], plse[seqs(i)]
        top = jnp.maximum(a, b)
        both = top + jnp.log2(jnp.exp2(a - top) + jnp.exp2(b - top))
        clse[seqs(i)] = both
        wa, wb = jnp.transpose(jnp.exp2(a - both)), jnp.transpose(jnp.exp2(b - both))
        for j in range(GO):
            for cc in range(chips):
                sl = slice(cc * rows, (cc + 1) * rows)
                x = o_all[k, cc, i * GO + j].astype(jnp.float32) * wa[sl, j:j + 1]
                y = prx[cc, i * GO + j].astype(jnp.float32) * wb[sl, j:j + 1]
                o_all[k, cc, i * GO + j] = (x + y).astype(jnp.bfloat16)

    def oreg(cc, i, part):
        if part is None:
            return o_all.at[k, cc, seqs(i)]
        return o_all.at[k, cc, pl.ds(i * GO + part * half, half)]

    def breg(side, i, part):
        return bbuf.at[side, pl.ds(i * GO + part * half, half)]

    def a_send(i):
        return [rcopy(oreg(cf, i, 0), abuf.at[0, pl.ds(i * half, half)], as_.at[0, i], ar.at[0, i], right),
                rcopy(oreg(cf, i, 1), abuf.at[1, pl.ds(i * half, half)], as_.at[1, i], ar.at[1, i], left),
                rcopy(clse.at[seqs(i)], alse.at[0, seqs(i)], as_.at[2, i], ar.at[2, i], right),
                rcopy(clse.at[seqs(i)], alse.at[1, seqs(i)], as_.at[3, i], ar.at[3, i], left)]

    def b_early(i):
        return [rcopy(oreg(cr, i, 1), breg(0, i, 1), bs.at[0, i], br.at[0, i], right),
                rcopy(oreg(cl, i, 0), breg(1, i, 0), bs.at[1, i], br.at[1, i], left)]

    def b_late(i):
        return [rcopy(oreg(cr, i, 0), breg(0, i, 0), bs.at[2, i], br.at[2, i], right),
                rcopy(oreg(cl, i, 1), breg(1, i, 1), bs.at[3, i], br.at[3, i], left),
                rcopy(nlse.at[seqs(i)], blse.at[0, seqs(i)], bs.at[4, i], br.at[4, i], right),
                rcopy(nlse.at[seqs(i)], blse.at[1, seqs(i)], bs.at[5, i], br.at[5, i], left)]

    seq_id = lax.broadcasted_iota(jnp.int32, (GO, lanes), 0)
    chip_id = lax.broadcasted_iota(jnp.int32, (GO, lanes), 1) // rows
    from_left = (seq_id < half) & (chip_id == cr)
    from_right = (seq_id >= half) & (chip_id == cl)

    def a_merge(i):
        for cp in a_send(i):
            cp.wait_recv()
        a = clse[seqs(i)]
        b = jnp.where(from_left, alse[0, seqs(i)], jnp.where(from_right, alse[1, seqs(i)], a))
        top = jnp.maximum(a, b)
        both = top + jnp.log2(jnp.exp2(a - top) + jnp.exp2(b - top))
        wt[0], wt[1] = jnp.transpose(jnp.exp2(a - both)), jnp.transpose(jnp.exp2(b - both))
        nlse[seqs(i)] = jnp.where(from_left | from_right, both, a)
        for side, cc in ((0, cr), (1, cl)):
            wa, wb = (wt[n, pl.ds(pl.multiple_of(cc * rows, rows), rows)] for n in range(2))
            for j in range(half):
                lane = side * half + j
                x = o_all[k, cc, i * GO + lane].astype(jnp.float32) * wa[:, lane:lane + 1]
                y = abuf[side, i * half + j].astype(jnp.float32) * wb[:, lane:lane + 1]
                o_all[k, cc, i * GO + lane] = (x + y).astype(jnp.bfloat16)
        for cp in b_late(i):
            cp.start()

    def out_copy(i):
        return pltpu.make_async_copy(o_all.at[k, c, seqs(i)], out_hbm.at[seqs(i)], out_sem.at[i])

    def final_merge(i):
        for cp in b_early(i) + b_late(i):
            cp.wait_recv()
        parts = [clse[seqs(i)], blse[0, seqs(i)], blse[1, seqs(i)]]
        top = functools.reduce(jnp.maximum, parts)
        total = top + jnp.log2(sum(jnp.exp2(x - top) for x in parts))
        for n, x in enumerate(parts):
            wt[n] = jnp.transpose(jnp.exp2(x - total))
        w = [wt[n, pl.ds(pl.multiple_of(c * rows, rows), rows)] for n in range(3)]
        for j in range(GO):
            b = i * GO + j
            x = o_all[k, c, b].astype(jnp.float32) * w[0][:, j:j + 1]
            x += bbuf[0, b].astype(jnp.float32) * w[1][:, j:j + 1]
            x += bbuf[1, b].astype(jnp.float32) * w[2][:, j:j + 1]
            o_all[k, c, b] = x.astype(jnp.bfloat16)
        out_copy(i).start()

    def ring_start(i):
        for cp in a_send(i) + b_early(i):
            cp.start()

    for j in range(AHEAD):
        for cp in q_own(j):
            cp.start()

    def step(j, carry):
        @pl.when(j < n_q)
        def _():
            q_arrival(0, j).wait_recv()
            q_arrival(1, j).wait_recv()
            for cp in q_relay(j):
                cp.start()

        @pl.when(j + AHEAD < n_q)
        def _():
            for cp in q_own(j + AHEAD):
                cp.start()

        @pl.when((j >= 1) & (j <= n_q))
        def _():
            q_arrival(3, j - 1).wait_recv()
            q_arrival(4, j - 1).wait_recv()
            for cp in q_far(j - 1):
                cp.start()

        @pl.when(j == HOLD)
        def _():
            lax.fori_loop(0, (HOLD - 3) // 2, lambda i, cc: (ring_start(i), cc)[1], 0)

        @pl.when(j >= 2)
        def _():
            s = j - 2
            for kind in (2, 5, 6, 7, 8):
                q_arrival(kind, s).wait_recv()
            lax.fori_loop(0, GQ, lambda n, cc: (attend(s * GQ + n), cc)[1], 0)
            i = s // 2

            @pl.when(s % 2 == 1)
            def _():
                for cp in d_send(i):
                    cp.start()

            @pl.when((s % 2 == 0) & (s > 0))
            def _():
                d_merge(i - 1)

                @pl.when(j >= HOLD)
                def _():
                    ring_start(i - 1)

        return carry

    lax.fori_loop(0, n_q + 2, step, 0)
    d_merge(n_o - 1)
    ring_start(n_o - 1)
    lax.fori_loop(0, n_o, lambda i, cc: (a_merge(i), cc)[1], 0)
    lax.fori_loop(0, n_o, lambda i, cc: (final_merge(i), cc)[1], 0)

    def drain_q(j, carry):
        for cp in q_own(j) + q_relay(j) + q_far(j):
            cp.wait_send()
        return carry

    def drain_o(i, carry):
        for cp in d_send(i) + a_send(i) + b_early(i) + b_late(i):
            cp.wait_send()
        out_copy(i).wait()
        return carry

    lax.fori_loop(0, n_q, drain_q, 0)
    lax.fori_loop(0, n_o, drain_o, 0)


def solution(mesh):
    group = mesh.shape['dcp']
    chips = group // CORES

    def local_step(q_blk, kv_blk, len_blk):
        batch, toks, heads, width = q_blk.shape
        npos = kv_blk.shape[1] * kv_blk.shape[2] * kv_blk.shape[3]
        rows, lanes = toks * heads, chips * toks * heads
        n_q, n_o = batch // GQ, batch // GO
        bf16, f32, dma = jnp.bfloat16, jnp.float32, pltpu.SemaphoreType.DMA
        any_space = pl.BlockSpec(memory_space=pl.ANY)
        out = pl.pallas_call(
            functools.partial(_kernel, (batch, toks, heads, npos, group)),
            out_shape=jax.ShapeDtypeStruct((batch, rows, LATENT), bf16),
            in_specs=[any_space, any_space, pl.BlockSpec(memory_space=pltpu.SMEM)],
            out_specs=any_space,
            scratch_shapes=[
                pltpu.VMEM((CORES, chips, batch, heads, toks * width), bf16),
                pltpu.VMEM((batch, toks, heads, ROPE), bf16),
                pltpu.VMEM((KV_SLOTS, npos, width), bf16),
                pltpu.VMEM((CORES, chips, batch, rows, LATENT), bf16),
                pltpu.VMEM((chips, batch, rows, LATENT), bf16),
                pltpu.VMEM((2, batch // 2, rows, LATENT), bf16),
                pltpu.VMEM((2, batch, rows, LATENT), bf16),
                pltpu.VMEM((CORES, batch, lanes), f32),
                pltpu.VMEM((batch, lanes), f32),
                pltpu.VMEM((batch, lanes), f32),
                pltpu.VMEM((2, batch, lanes), f32),
                pltpu.VMEM((batch, lanes), f32),
                pltpu.VMEM((2, batch, lanes), f32),
                pltpu.VMEM((3, lanes, GO), f32),
                dma((toks + 1,)), dma((KV_SLOTS,)), dma((n_o,)),
                dma((9, n_q)), dma((9, n_q)),
                dma((2, n_o)), dma((2, n_o)),
                dma((4, n_o)), dma((4, n_o)),
                dma((6, n_o)), dma((6, n_o)),
            ],
            compiler_params=pltpu.CompilerParams(collective_id=0, has_side_effects=True, vmem_limit_bytes=67_043_328),
            name='mla_ring',
        )(q_blk, kv_blk.reshape(batch, npos, width), len_blk)
        return out.reshape(batch, toks, heads, LATENT)

    return jax.shard_map(local_step, mesh=mesh, in_specs=(P('dp', None, 'dcp', None), P('dp', None, 'dcp', None, None), P('dp')),
                         out_specs=P('dp', None, 'dcp', None), check_vma=False)
```

```python
import functools
import math

import jax
import jax.numpy as jnp
from jax import lax
from jax.experimental import pallas as pl
from jax.experimental.pallas import tpu as pltpu
from jax.sharding import PartitionSpec as P

LATENT = 512
ROPE = 64
NOPE = 128
PAGE = 64
CORES = 2
SCALE2 = (NOPE + ROPE) ** -0.5 * math.log2(math.e)

GQ = 4
GO = 8
KV_SLOTS = 4
UNROLL = 2
AHEAD = 2


def _kernel(sizes, q_hbm, kv_hbm, len_ref, out_hbm,
            qall, rope_in, kvb, o_all, prx, abuf, bbuf,
            lse_all, plse, clse, alse, nlse, blse, wt,
            load_sem, kv_sem, out_sem, qs, qr, ds, dr, as_, ar, bs, br):
    batch, toks, heads, npos, group = sizes
    chips = group // CORES
    rows = toks * heads
    half = GO // 2
    n_q, n_o = batch // GQ, batch // GO
    me = lax.axis_index('dcp')
    c, k = me // CORES, me % CORES
    ok = 1 - k
    cr, cl, cf = (c + 1) % chips, (c + chips - 1) % chips, (c + 2) % chips
    right, left, partner = cr * CORES + k, cl * CORES + k, c * CORES + ok

    barrier = pltpu.get_barrier_semaphore()
    for other in (right, left, partner):
        pl.semaphore_signal(barrier, inc=1, device_id={'dcp': other}, device_id_type=pl.DeviceIdType.MESH)

    def rcopy(src, dst, send, recv, dev):
        return pltpu.make_async_remote_copy(src_ref=src, dst_ref=dst, send_sem=send, recv_sem=recv,
                                            device_id={'dcp': dev}, device_id_type=pl.DeviceIdType.MESH)

    loads = [pltpu.make_async_copy(q_hbm.at[:, t, :, 0:LATENT], qall.at[k, c, :, :, t * LATENT:(t + 1) * LATENT], load_sem.at[t])
             for t in range(toks)]
    loads.append(pltpu.make_async_copy(q_hbm.at[:, :, :, LATENT:LATENT + ROPE], rope_in, load_sem.at[toks]))
    for cp in loads[::-1]:
        cp.start()
    loads[toks].wait()
    qall[k, c, :, :, toks * LATENT:] = jnp.concatenate([rope_in[:, t] for t in range(toks)], axis=-1)
    for t in range(toks):
        loads[t].wait()
    pl.semaphore_wait(barrier, 3)

    def kv_copy(b):
        slot = lax.rem(b, KV_SLOTS)
        return pltpu.make_async_copy(kv_hbm.at[b], kvb.at[slot], kv_sem.at[slot])

    def qreg(kk, cc, b0, n):
        return qall.at[kk, cc, pl.ds(b0, n)]

    def q_own(j):
        r = qreg(k, c, j * GQ, GQ)
        return [rcopy(r, r, qs.at[0, j], qr.at[0, j], right), rcopy(r, r, qs.at[1, j], qr.at[1, j], left),
                rcopy(r, r, qs.at[2, j], qr.at[2, j], partner)]

    def q_relay(j):
        lr, rr = qreg(k, cl, j * GQ, GQ), qreg(k, cr, j * GQ, GQ)
        lh, rh = qreg(k, cl, j * GQ, GQ // 2), qreg(k, cr, j * GQ + GQ // 2, GQ // 2)
        return [rcopy(lh, lh, qs.at[3, j], qr.at[3, j], right), rcopy(rh, rh, qs.at[4, j], qr.at[4, j], left),
                rcopy(lr, lr, qs.at[5, j], qr.at[5, j], partner), rcopy(rr, rr, qs.at[6, j], qr.at[6, j], partner)]

    def q_far(j):
        f0, f1 = qreg(k, cf, j * GQ, GQ // 2), qreg(k, cf, j * GQ + GQ // 2, GQ // 2)
        return [rcopy(f0, f0, qs.at[7, j], qr.at[7, j], partner), rcopy(f1, f1, qs.at[8, j], qr.at[8, j], partner)]

    def q_arrival(kind, j):
        full, h0, h1 = (j * GQ, GQ), (j * GQ, GQ // 2), (j * GQ + GQ // 2, GQ // 2)
        kk, cc, span = [(k, cl, full), (k, cr, full), (ok, c, full), (k, cf, h0), (k, cf, h1),
                        (ok, cl, full), (ok, cr, full), (ok, cf, h0), (ok, cf, h1)][kind]
        r = qreg(kk, cc, *span)
        return rcopy(r, r, qs.at[kind, j], qr.at[kind, j], partner)

    row_tok = (lax.broadcasted_iota(jnp.int32, (CORES * chips * rows, 1), 0) // heads) % toks
    key = lax.broadcasted_iota(jnp.int32, (1, npos), 1)
    pos = ((key // PAGE) * group + me) * PAGE + key % PAGE
    lanes = chips * rows
    eye = lax.broadcasted_iota(jnp.int32, (lanes, lanes), 0) == lax.broadcasted_iota(jnp.int32, (lanes, lanes), 1)

    def scores(b):
        kv_copy(b).wait()
        slot = lax.rem(b, KV_SLOTS)
        q = qall[:, :, b].reshape(CORES * chips, heads, toks * (LATENT + ROPE))
        lat = jnp.stack([q[:, :, t * LATENT:(t + 1) * LATENT] for t in range(toks)], axis=1).reshape(-1, LATENT)
        rope0 = toks * LATENT
        rope = jnp.stack([q[:, :, rope0 + t * ROPE:rope0 + (t + 1) * ROPE] for t in range(toks)], axis=1).reshape(-1, ROPE)
        q_rows = jnp.concatenate([lat, rope], axis=-1)
        return lax.dot_general(q_rows, kvb[slot], (((1,), (1,)), ((), ())), preferred_element_type=jnp.float32)

    def weights(b, s):
        s = jnp.where(pos <= len_ref[b] - toks + row_tok, s, -jnp.inf)
        m = jnp.max(s, axis=-1, keepdims=True)
        p = jnp.exp2((s - m) * SCALE2)
        return m, jnp.sum(p, axis=-1, keepdims=True), p.astype(jnp.bfloat16)

    def output(b, m, l, p):
        slot = lax.rem(b, KV_SLOTS)
        o = jnp.dot(p, kvb[slot, :, 0:LATENT], preferred_element_type=jnp.float32)
        o = (o * (1.0 / l)).astype(jnp.bfloat16)
        o_all[:, :, b] = o.reshape(CORES, chips, rows, LATENT)
        lse = m * SCALE2 + jnp.log2(l)
        for kk in range(CORES):
            col = lse[kk * lanes:(kk + 1) * lanes]
            lse_all[kk, pl.ds(b, 1)] = jnp.sum(jnp.where(eye, col, 0.0), axis=0, keepdims=True)

    def attend(b0):
        bs_ = [b0 + u for u in range(UNROLL)]
        ss = [scores(b) for b in bs_]
        for b, s in zip(bs_, ss):
            output(b, *weights(b, s))
        for b in bs_:
            @pl.when(b + KV_SLOTS < batch)
            def _():
                kv_copy(b + KV_SLOTS).start()

    def seqs(i, n=GO):
        return pl.ds(pl.multiple_of(i * n, n), n)

    def d_send(i):
        return [rcopy(o_all.at[ok, :, seqs(i)], prx.at[:, seqs(i)], ds.at[0, i], dr.at[0, i], partner),
                rcopy(lse_all.at[ok, seqs(i)], plse.at[seqs(i)], ds.at[1, i], dr.at[1, i], partner)]

    def d_merge(i):
        for cp in d_send(i):
            cp.wait_recv()
        a, b = lse_all[k, seqs(i)], plse[seqs(i)]
        top = jnp.maximum(a, b)
        both = top + jnp.log2(jnp.exp2(a - top) + jnp.exp2(b - top))
        clse[seqs(i)] = both
        wa, wb = jnp.transpose(jnp.exp2(a - both)), jnp.transpose(jnp.exp2(b - both))
        for j in range(GO):
            for cc in range(chips):
                sl = slice(cc * rows, (cc + 1) * rows)
                x = o_all[k, cc, i * GO + j].astype(jnp.float32) * wa[sl, j:j + 1]
                y = prx[cc, i * GO + j].astype(jnp.float32) * wb[sl, j:j + 1]
                o_all[k, cc, i * GO + j] = (x + y).astype(jnp.bfloat16)

    def oreg(cc, i, part):
        if part is None:
            return o_all.at[k, cc, seqs(i)]
        return o_all.at[k, cc, pl.ds(i * GO + part * half, half)]

    def breg(side, i, part):
        return bbuf.at[side, pl.ds(i * GO + part * half, half)]

    def a_send(i):
        return [rcopy(oreg(cf, i, 0), abuf.at[0, pl.ds(i * half, half)], as_.at[0, i], ar.at[0, i], right),
                rcopy(oreg(cf, i, 1), abuf.at[1, pl.ds(i * half, half)], as_.at[1, i], ar.at[1, i], left),
                rcopy(clse.at[seqs(i)], alse.at[0, seqs(i)], as_.at[2, i], ar.at[2, i], right),
                rcopy(clse.at[seqs(i)], alse.at[1, seqs(i)], as_.at[3, i], ar.at[3, i], left)]

    def b_early(i):
        return [rcopy(oreg(cr, i, 1), breg(0, i, 1), bs.at[0, i], br.at[0, i], right),
                rcopy(oreg(cl, i, 0), breg(1, i, 0), bs.at[1, i], br.at[1, i], left)]

    def b_late(i):
        return [rcopy(oreg(cr, i, 0), breg(0, i, 0), bs.at[2, i], br.at[2, i], right),
                rcopy(oreg(cl, i, 1), breg(1, i, 1), bs.at[3, i], br.at[3, i], left),
                rcopy(nlse.at[seqs(i)], blse.at[0, seqs(i)], bs.at[4, i], br.at[4, i], right),
                rcopy(nlse.at[seqs(i)], blse.at[1, seqs(i)], bs.at[5, i], br.at[5, i], left)]

    seq_id = lax.broadcasted_iota(jnp.int32, (GO, lanes), 0)
    chip_id = lax.broadcasted_iota(jnp.int32, (GO, lanes), 1) // rows
    from_left = (seq_id < half) & (chip_id == cr)
    from_right = (seq_id >= half) & (chip_id == cl)

    def a_merge(i):
        for cp in a_send(i):
            cp.wait_recv()
        a = clse[seqs(i)]
        b = jnp.where(from_left, alse[0, seqs(i)], jnp.where(from_right, alse[1, seqs(i)], a))
        top = jnp.maximum(a, b)
        both = top + jnp.log2(jnp.exp2(a - top) + jnp.exp2(b - top))
        wt[0], wt[1] = jnp.transpose(jnp.exp2(a - both)), jnp.transpose(jnp.exp2(b - both))
        nlse[seqs(i)] = jnp.where(from_left | from_right, both, a)
        for side, cc in ((0, cr), (1, cl)):
            wa, wb = (wt[n, pl.ds(pl.multiple_of(cc * rows, rows), rows)] for n in range(2))
            for j in range(half):
                lane = side * half + j
                x = o_all[k, cc, i * GO + lane].astype(jnp.float32) * wa[:, lane:lane + 1]
                y = abuf[side, i * half + j].astype(jnp.float32) * wb[:, lane:lane + 1]
                o_all[k, cc, i * GO + lane] = (x + y).astype(jnp.bfloat16)
        for cp in b_late(i):
            cp.start()

    def out_copy(i):
        return pltpu.make_async_copy(o_all.at[k, c, seqs(i)], out_hbm.at[seqs(i)], out_sem.at[i])

    def final_merge(i):
        for cp in b_early(i) + b_late(i):
            cp.wait_recv()
        parts = [clse[seqs(i)], blse[0, seqs(i)], blse[1, seqs(i)]]
        top = functools.reduce(jnp.maximum, parts)
        total = top + jnp.log2(sum(jnp.exp2(x - top) for x in parts))
        for n, x in enumerate(parts):
            wt[n] = jnp.transpose(jnp.exp2(x - total))
        w = [wt[n, pl.ds(pl.multiple_of(c * rows, rows), rows)] for n in range(3)]
        for j in range(GO):
            b = i * GO + j
            x = o_all[k, c, b].astype(jnp.float32) * w[0][:, j:j + 1]
            x += bbuf[0, b].astype(jnp.float32) * w[1][:, j:j + 1]
            x += bbuf[1, b].astype(jnp.float32) * w[2][:, j:j + 1]
            o_all[k, c, b] = x.astype(jnp.bfloat16)
        out_copy(i).start()

    def start(copies):
        for cp in copies:
            cp.start()

    def ring_start(lo, hi):
        lax.fori_loop(lo, hi, lambda i, carry: (start(a_send(i) + b_early(i)), carry)[1], 0)

    for j in range(AHEAD):
        for cp in q_own(j):
            cp.start()
    for b in range(KV_SLOTS):
        kv_copy(b).start()

    def step(j, carry):
        @pl.when(j < n_q)
        def _():
            q_arrival(0, j).wait_recv()
            q_arrival(1, j).wait_recv()
            for cp in q_relay(j):
                cp.start()

        @pl.when(j + AHEAD < n_q)
        def _():
            for cp in q_own(j + AHEAD):
                cp.start()

        @pl.when((j >= 1) & (j <= n_q))
        def _():
            q_arrival(3, j - 1).wait_recv()
            q_arrival(4, j - 1).wait_recv()
            for cp in q_far(j - 1):
                cp.start()

        @pl.when(j == n_q - 2)
        def _():
            start(a_send(0))

        @pl.when(j == n_q - 1)
        def _():
            start(b_early(0))
            ring_start(1, n_o // 2)

        @pl.when(j == n_q)
        def _():
            ring_start(n_o // 2, n_o - 2)

        @pl.when(j == n_q + 1)
        def _():
            ring_start(n_o - 2, n_o - 1)

        @pl.when(j >= 2)
        def _():
            s = j - 2
            for kind in (2, 5, 6, 7, 8):
                q_arrival(kind, s).wait_recv()
            lax.fori_loop(0, GQ // UNROLL, lambda n, cc: (attend(s * GQ + n * UNROLL), cc)[1], 0)
            i = s // 2

            @pl.when(s % 2 == 1)
            def _():
                for cp in d_send(i):
                    cp.start()

            @pl.when((s % 2 == 0) & (s > 0))
            def _():
                d_merge(i - 1)

        return carry

    lax.fori_loop(0, n_q + 2, step, 0)
    d_merge(n_o - 1)
    ring_start(n_o - 1, n_o)
    lax.fori_loop(0, n_o, lambda i, cc: (a_merge(i), cc)[1], 0)
    lax.fori_loop(0, n_o, lambda i, cc: (final_merge(i), cc)[1], 0)

    def drain_q(j, carry):
        for cp in q_own(j) + q_relay(j) + q_far(j):
            cp.wait_send()
        return carry

    def drain_o(i, carry):
        for cp in d_send(i) + a_send(i) + b_early(i) + b_late(i):
            cp.wait_send()
        out_copy(i).wait()
        return carry

    lax.fori_loop(0, n_q, drain_q, 0)
    lax.fori_loop(0, n_o, drain_o, 0)


def solution(mesh):
    group = mesh.shape['dcp']
    chips = group // CORES

    def local_step(q_blk, kv_blk, len_blk):
        batch, toks, heads, width = q_blk.shape
        npos = kv_blk.shape[1] * kv_blk.shape[2] * kv_blk.shape[3]
        rows, lanes = toks * heads, chips * toks * heads
        n_q, n_o = batch // GQ, batch // GO
        bf16, f32, dma = jnp.bfloat16, jnp.float32, pltpu.SemaphoreType.DMA
        any_space = pl.BlockSpec(memory_space=pl.ANY)
        out = pl.pallas_call(
            functools.partial(_kernel, (batch, toks, heads, npos, group)),
            out_shape=jax.ShapeDtypeStruct((batch, rows, LATENT), bf16),
            in_specs=[any_space, any_space, pl.BlockSpec(memory_space=pltpu.SMEM)],
            out_specs=any_space,
            scratch_shapes=[
                pltpu.VMEM((CORES, chips, batch, heads, toks * width), bf16),
                pltpu.VMEM((batch, toks, heads, ROPE), bf16),
                pltpu.VMEM((KV_SLOTS, npos, width), bf16),
                pltpu.VMEM((CORES, chips, batch, rows, LATENT), bf16),
                pltpu.VMEM((chips, batch, rows, LATENT), bf16),
                pltpu.VMEM((2, batch // 2, rows, LATENT), bf16),
                pltpu.VMEM((2, batch, rows, LATENT), bf16),
                pltpu.VMEM((CORES, batch, lanes), f32),
                pltpu.VMEM((batch, lanes), f32),
                pltpu.VMEM((batch, lanes), f32),
                pltpu.VMEM((2, batch, lanes), f32),
                pltpu.VMEM((batch, lanes), f32),
                pltpu.VMEM((2, batch, lanes), f32),
                pltpu.VMEM((3, lanes, GO), f32),
                dma((toks + 1,)), dma((KV_SLOTS,)), dma((n_o,)),
                dma((9, n_q)), dma((9, n_q)),
                dma((2, n_o)), dma((2, n_o)),
                dma((4, n_o)), dma((4, n_o)),
                dma((6, n_o)), dma((6, n_o)),
            ],
            compiler_params=pltpu.CompilerParams(collective_id=0, has_side_effects=True, vmem_limit_bytes=67_043_328),
            name='mla_ring',
        )(q_blk, kv_blk.reshape(batch, npos, width), len_blk)
        return out.reshape(batch, toks, heads, LATENT)

    return jax.shard_map(local_step, mesh=mesh, in_specs=(P('dp', None, 'dcp', None), P('dp', None, 'dcp', None, None), P('dp')),
                         out_specs=P('dp', None, 'dcp', None), check_vma=False)
```

```python
import functools
import math

import jax
import jax.numpy as jnp
from jax import lax
from jax.experimental import pallas as pl
from jax.experimental.pallas import tpu as pltpu
from jax.sharding import PartitionSpec as P

LATENT = 512
ROPE = 64
NOPE = 128
PAGE = 64
CORES = 2
SCALE2 = (NOPE + ROPE) ** -0.5 * math.log2(math.e)

GQ = 4
GO = 8
KV_SLOTS = 4
UNROLL = 2
AHEAD = 2


def _kernel(sizes, q_hbm, kv_hbm, len_ref, out_ref,
            qall, rope_in, kvb, o_all, prx, abuf, bbuf,
            lse_all, plse, clse, alse, nlse, blse, wt,
            load_sem, kv_sem, qs, qr, ds, dr, as_, ar, bs, br):
    batch, toks, heads, npos, group = sizes
    chips = group // CORES
    rows = toks * heads
    half = GO // 2
    n_q, n_o = batch // GQ, batch // GO
    me = lax.axis_index('dcp')
    c, k = me // CORES, me % CORES
    ok = 1 - k
    cr, cl, cf = (c + 1) % chips, (c + chips - 1) % chips, (c + 2) % chips
    right, left, partner = cr * CORES + k, cl * CORES + k, c * CORES + ok

    barrier = pltpu.get_barrier_semaphore()
    for other in (right, left, partner):
        pl.semaphore_signal(barrier, inc=1, device_id={'dcp': other}, device_id_type=pl.DeviceIdType.MESH)

    def rcopy(src, dst, send, recv, dev):
        return pltpu.make_async_remote_copy(src_ref=src, dst_ref=dst, send_sem=send, recv_sem=recv,
                                            device_id={'dcp': dev}, device_id_type=pl.DeviceIdType.MESH)

    spans = ((0, AHEAD * GQ), (AHEAD * GQ, batch))

    def q_loads(n):
        span = slice(*spans[n])
        lat = [pltpu.make_async_copy(q_hbm.at[span, t, :, 0:LATENT], qall.at[k, c, span, :, t * LATENT:(t + 1) * LATENT], load_sem.at[n, t])
               for t in range(toks)]
        return lat, pltpu.make_async_copy(q_hbm.at[span, :, :, LATENT:LATENT + ROPE], rope_in.at[span], load_sem.at[n, toks])

    def q_ready(n):
        lat, rope = q_loads(n)
        span = slice(*spans[n])
        rope.wait()
        qall[k, c, span, :, toks * LATENT:] = jnp.concatenate([rope_in[span, t] for t in range(toks)], axis=-1)
        for cp in lat:
            cp.wait()

    def start(copies):
        for cp in copies:
            cp.start()

    for n in range(2):
        lat, rope = q_loads(n)
        start([rope] + lat)

    def kv_copy(b):
        slot = lax.rem(b, KV_SLOTS)
        return pltpu.make_async_copy(kv_hbm.at[b], kvb.at[slot], kv_sem.at[slot])

    def qreg(kk, cc, b0, n):
        return qall.at[kk, cc, pl.ds(b0, n)]

    def q_own(j):
        r = qreg(k, c, j * GQ, GQ)
        return [rcopy(r, r, qs.at[0, j], qr.at[0, j], right), rcopy(r, r, qs.at[1, j], qr.at[1, j], left),
                rcopy(r, r, qs.at[2, j], qr.at[2, j], partner)]

    def q_relay(j):
        lr, rr = qreg(k, cl, j * GQ, GQ), qreg(k, cr, j * GQ, GQ)
        lh, rh = qreg(k, cl, j * GQ, GQ // 2), qreg(k, cr, j * GQ + GQ // 2, GQ // 2)
        return [rcopy(lh, lh, qs.at[3, j], qr.at[3, j], right), rcopy(rh, rh, qs.at[4, j], qr.at[4, j], left),
                rcopy(lr, lr, qs.at[5, j], qr.at[5, j], partner), rcopy(rr, rr, qs.at[6, j], qr.at[6, j], partner)]

    def q_far(j):
        f0, f1 = qreg(k, cf, j * GQ, GQ // 2), qreg(k, cf, j * GQ + GQ // 2, GQ // 2)
        return [rcopy(f0, f0, qs.at[7, j], qr.at[7, j], partner), rcopy(f1, f1, qs.at[8, j], qr.at[8, j], partner)]

    def q_arrival(kind, j):
        full, h0, h1 = (j * GQ, GQ), (j * GQ, GQ // 2), (j * GQ + GQ // 2, GQ // 2)
        kk, cc, span = [(k, cl, full), (k, cr, full), (ok, c, full), (k, cf, h0), (k, cf, h1),
                        (ok, cl, full), (ok, cr, full), (ok, cf, h0), (ok, cf, h1)][kind]
        r = qreg(kk, cc, *span)
        return rcopy(r, r, qs.at[kind, j], qr.at[kind, j], partner)

    row_tok = (lax.broadcasted_iota(jnp.int32, (CORES * chips * rows, 1), 0) // heads) % toks
    key = lax.broadcasted_iota(jnp.int32, (1, npos), 1)
    pos = ((key // PAGE) * group + me) * PAGE + key % PAGE
    lanes = chips * rows
    eye = lax.broadcasted_iota(jnp.int32, (lanes, lanes), 0) == lax.broadcasted_iota(jnp.int32, (lanes, lanes), 1)

    def scores(b):
        slot = lax.rem(b, KV_SLOTS)
        q = qall[:, :, b].reshape(CORES * chips, heads, toks * (LATENT + ROPE))
        lat = jnp.stack([q[:, :, t * LATENT:(t + 1) * LATENT] for t in range(toks)], axis=1).reshape(-1, LATENT)
        rope0 = toks * LATENT
        rope = jnp.stack([q[:, :, rope0 + t * ROPE:rope0 + (t + 1) * ROPE] for t in range(toks)], axis=1).reshape(-1, ROPE)
        q_rows = jnp.concatenate([lat, rope], axis=-1)
        return lax.dot_general(q_rows, kvb[slot], (((1,), (1,)), ((), ())), preferred_element_type=jnp.float32)

    def weights(b, s):
        s = jnp.where(pos <= len_ref[b] - toks + row_tok, s, -jnp.inf)
        m = jnp.max(s, axis=-1, keepdims=True)
        p = jnp.exp2((s - m) * SCALE2)
        return m, jnp.sum(p, axis=-1, keepdims=True), p.astype(jnp.bfloat16)

    def output(b, m, l, p):
        slot = lax.rem(b, KV_SLOTS)
        o = jnp.dot(p, kvb[slot, :, 0:LATENT], preferred_element_type=jnp.float32)
        o = (o * (1.0 / l)).astype(jnp.bfloat16)
        o_all[:, :, b] = o.reshape(CORES, chips, rows, LATENT)
        lse = m * SCALE2 + jnp.log2(l)
        for kk in range(CORES):
            col = lse[kk * lanes:(kk + 1) * lanes]
            lse_all[kk, pl.ds(b, 1)] = jnp.sum(jnp.where(eye, col, 0.0), axis=0, keepdims=True)

    def attend(b0):
        bs_ = [b0 + u for u in range(UNROLL)]
        for b in bs_:
            kv_copy(b).wait()
        s = scores(bs_[0])
        for b in bs_:
            following = scores(b + 1) if b is not bs_[-1] else None
            output(b, *weights(b, s))
            s = following
        for b in bs_:
            @pl.when(b + KV_SLOTS < batch)
            def _():
                kv_copy(b + KV_SLOTS).start()

    def seqs(i, n=GO):
        return pl.ds(pl.multiple_of(i * n, n), n)

    def d_send(i):
        return [rcopy(o_all.at[ok, :, seqs(i)], prx.at[:, seqs(i)], ds.at[0, i], dr.at[0, i], partner),
                rcopy(lse_all.at[ok, seqs(i)], plse.at[seqs(i)], ds.at[1, i], dr.at[1, i], partner)]

    def d_merge(i):
        for cp in d_send(i):
            cp.wait_recv()
        a, b = lse_all[k, seqs(i)], plse[seqs(i)]
        top = jnp.maximum(a, b)
        both = top + jnp.log2(jnp.exp2(a - top) + jnp.exp2(b - top))
        clse[seqs(i)] = both
        wa, wb = jnp.transpose(jnp.exp2(a - both)), jnp.transpose(jnp.exp2(b - both))
        for j in range(GO):
            for cc in range(chips):
                sl = slice(cc * rows, (cc + 1) * rows)
                x = o_all[k, cc, i * GO + j].astype(jnp.float32) * wa[sl, j:j + 1]
                y = prx[cc, i * GO + j].astype(jnp.float32) * wb[sl, j:j + 1]
                o_all[k, cc, i * GO + j] = (x + y).astype(jnp.bfloat16)

    def oreg(cc, i, part):
        if part is None:
            return o_all.at[k, cc, seqs(i)]
        return o_all.at[k, cc, pl.ds(i * GO + part * half, half)]

    def breg(side, i, part):
        return bbuf.at[side, pl.ds(i * GO + part * half, half)]

    def a_send(i):
        return [rcopy(oreg(cf, i, 0), abuf.at[0, pl.ds(i * half, half)], as_.at[0, i], ar.at[0, i], right),
                rcopy(oreg(cf, i, 1), abuf.at[1, pl.ds(i * half, half)], as_.at[1, i], ar.at[1, i], left),
                rcopy(clse.at[seqs(i)], alse.at[0, seqs(i)], as_.at[2, i], ar.at[2, i], right),
                rcopy(clse.at[seqs(i)], alse.at[1, seqs(i)], as_.at[3, i], ar.at[3, i], left)]

    def b_early(i):
        return [rcopy(oreg(cr, i, 1), breg(0, i, 1), bs.at[0, i], br.at[0, i], right),
                rcopy(oreg(cl, i, 0), breg(1, i, 0), bs.at[1, i], br.at[1, i], left)]

    def b_late(i):
        return [rcopy(oreg(cr, i, 0), breg(0, i, 0), bs.at[2, i], br.at[2, i], right),
                rcopy(oreg(cl, i, 1), breg(1, i, 1), bs.at[3, i], br.at[3, i], left),
                rcopy(nlse.at[seqs(i)], blse.at[0, seqs(i)], bs.at[4, i], br.at[4, i], right),
                rcopy(nlse.at[seqs(i)], blse.at[1, seqs(i)], bs.at[5, i], br.at[5, i], left)]

    seq_id = lax.broadcasted_iota(jnp.int32, (GO, lanes), 0)
    chip_id = lax.broadcasted_iota(jnp.int32, (GO, lanes), 1) // rows
    from_left = (seq_id < half) & (chip_id == cr)
    from_right = (seq_id >= half) & (chip_id == cl)

    def a_merge(i):
        for cp in a_send(i):
            cp.wait_recv()
        a = clse[seqs(i)]
        b = jnp.where(from_left, alse[0, seqs(i)], jnp.where(from_right, alse[1, seqs(i)], a))
        top = jnp.maximum(a, b)
        both = top + jnp.log2(jnp.exp2(a - top) + jnp.exp2(b - top))
        wt[0], wt[1] = jnp.transpose(jnp.exp2(a - both)), jnp.transpose(jnp.exp2(b - both))
        nlse[seqs(i)] = jnp.where(from_left | from_right, both, a)
        for side, cc in ((0, cr), (1, cl)):
            wa, wb = (wt[n, pl.ds(pl.multiple_of(cc * rows, rows), rows)] for n in range(2))
            for j in range(half):
                lane = side * half + j
                x = o_all[k, cc, i * GO + lane].astype(jnp.float32) * wa[:, lane:lane + 1]
                y = abuf[side, i * half + j].astype(jnp.float32) * wb[:, lane:lane + 1]
                o_all[k, cc, i * GO + lane] = (x + y).astype(jnp.bfloat16)
        start(b_late(i))

    def final_merge(i):
        for cp in b_early(i) + b_late(i):
            cp.wait_recv()
        sent(b_late(i))
        parts = [clse[seqs(i)], blse[0, seqs(i)], blse[1, seqs(i)]]
        top = functools.reduce(jnp.maximum, parts)
        total = top + jnp.log2(sum(jnp.exp2(x - top) for x in parts))
        for n, x in enumerate(parts):
            wt[n] = jnp.transpose(jnp.exp2(x - total))
        w = [wt[n, pl.ds(pl.multiple_of(c * rows, rows), rows)] for n in range(3)]
        for j in range(GO):
            b = i * GO + j
            x = o_all[k, c, b].astype(jnp.float32) * w[0][:, j:j + 1]
            x += bbuf[0, b].astype(jnp.float32) * w[1][:, j:j + 1]
            x += bbuf[1, b].astype(jnp.float32) * w[2][:, j:j + 1]
            out_ref[b] = x.astype(jnp.bfloat16)

    def sent(copies):
        for cp in copies:
            cp.wait_send()

    def ring_start(lo, hi):
        lax.fori_loop(lo, hi, lambda i, carry: (start(a_send(i) + b_early(i)), carry)[1], 0)

    q_ready(0)
    pl.semaphore_wait(barrier, 3)
    for j in range(AHEAD):
        start(q_own(j))
    for b in range(KV_SLOTS):
        kv_copy(b).start()
    q_ready(1)

    def step(j, carry):
        @pl.when(j < n_q)
        def _():
            q_arrival(0, j).wait_recv()
            q_arrival(1, j).wait_recv()
            for cp in q_relay(j):
                cp.start()

        @pl.when(j + AHEAD < n_q)
        def _():
            for cp in q_own(j + AHEAD):
                cp.start()

        @pl.when((j >= 1) & (j <= n_q))
        def _():
            q_arrival(3, j - 1).wait_recv()
            q_arrival(4, j - 1).wait_recv()
            for cp in q_far(j - 1):
                cp.start()

        @pl.when(j == n_q - 2)
        def _():
            start(a_send(0))

        @pl.when(j == n_q - 1)
        def _():
            start(b_early(0))
            ring_start(1, n_o // 2)

        @pl.when(j == n_q)
        def _():
            ring_start(n_o // 2, n_o - 2)

        @pl.when(j == n_q + 1)
        def _():
            ring_start(n_o - 2, n_o - 1)

        @pl.when(j >= 2)
        def _():
            s = j - 2
            for kind in (2, 5, 6, 7, 8):
                q_arrival(kind, s).wait_recv()
            lax.fori_loop(0, GQ // UNROLL, lambda n, cc: (attend(s * GQ + n * UNROLL), cc)[1], 0)
            i = s // 2

            @pl.when(s % 2 == 1)
            def _():
                for cp in d_send(i):
                    cp.start()

            @pl.when((s % 2 == 0) & (s > 0))
            def _():
                d_merge(i - 1)

        return carry

    lax.fori_loop(0, n_q + 2, step, 0)
    d_merge(n_o - 1)
    ring_start(n_o - 1, n_o)
    lax.fori_loop(0, n_q, lambda j, cc: (sent(q_own(j) + q_relay(j) + q_far(j)), cc)[1], 0)
    lax.fori_loop(0, n_o, lambda i, cc: (a_merge(i), cc)[1], 0)
    lax.fori_loop(0, n_o, lambda i, cc: (sent(d_send(i) + a_send(i) + b_early(i)), cc)[1], 0)
    lax.fori_loop(0, n_o, lambda i, cc: (final_merge(i), cc)[1], 0)


def solution(mesh):
    group = mesh.shape['dcp']
    chips = group // CORES

    def local_step(q_blk, kv_blk, len_blk):
        batch, toks, heads, width = q_blk.shape
        npos = kv_blk.shape[1] * kv_blk.shape[2] * kv_blk.shape[3]
        rows, lanes = toks * heads, chips * toks * heads
        n_q, n_o = batch // GQ, batch // GO
        bf16, f32, dma = jnp.bfloat16, jnp.float32, pltpu.SemaphoreType.DMA
        any_space = pl.BlockSpec(memory_space=pl.ANY)
        out = pl.pallas_call(
            functools.partial(_kernel, (batch, toks, heads, npos, group)),
            out_shape=pltpu.VMEM((batch, rows, LATENT), bf16),
            in_specs=[any_space, any_space, pl.BlockSpec(memory_space=pltpu.SMEM)],
            out_specs=pl.BlockSpec(memory_space=pltpu.VMEM),
            scratch_shapes=[
                pltpu.VMEM((CORES, chips, batch, heads, toks * width), bf16),
                pltpu.VMEM((batch, toks, heads, ROPE), bf16),
                pltpu.VMEM((KV_SLOTS, npos, width), bf16),
                pltpu.VMEM((CORES, chips, batch, rows, LATENT), bf16),
                pltpu.VMEM((chips, batch, rows, LATENT), bf16),
                pltpu.VMEM((2, batch // 2, rows, LATENT), bf16),
                pltpu.VMEM((2, batch, rows, LATENT), bf16),
                pltpu.VMEM((CORES, batch, lanes), f32),
                pltpu.VMEM((batch, lanes), f32),
                pltpu.VMEM((batch, lanes), f32),
                pltpu.VMEM((2, batch, lanes), f32),
                pltpu.VMEM((batch, lanes), f32),
                pltpu.VMEM((2, batch, lanes), f32),
                pltpu.VMEM((3, lanes, GO), f32),
                dma((2, toks + 1)), dma((KV_SLOTS,)),
                dma((9, n_q)), dma((9, n_q)),
                dma((2, n_o)), dma((2, n_o)),
                dma((4, n_o)), dma((4, n_o)),
                dma((6, n_o)), dma((6, n_o)),
            ],
            compiler_params=pltpu.CompilerParams(collective_id=0, has_side_effects=True, vmem_limit_bytes=63_000_000),
            name='mla_ring',
        )(q_blk, kv_blk.reshape(batch, npos, width), len_blk)
        return out.reshape(batch, toks, heads, LATENT)

    return jax.shard_map(local_step, mesh=mesh, in_specs=(P('dp', None, 'dcp', None), P('dp', None, 'dcp', None, None), P('dp')),
                         out_specs=P('dp', None, 'dcp', None), check_vma=False)
```

```python
import functools
import math

import jax
import jax.numpy as jnp
from jax import lax
from jax.experimental import pallas as pl
from jax.experimental.pallas import tpu as pltpu
from jax.sharding import PartitionSpec as P

LATENT = 512
ROPE = 64
NOPE = 128
PAGE = 64
CORES = 2
SCALE2 = (NOPE + ROPE) ** -0.5 * math.log2(math.e)

GQ = 4
GO = 8
KV_SLOTS = 4
UNROLL = 2
AHEAD = 3


def _kernel(sizes, q_hbm, kv_hbm, len_ref, out_ref,
            qall, rope_in, kvb, o_all, prx, abuf, bbuf,
            lse_all, plse, clse, asnd, alse, bsnd, blse,
            load_sem, kv_sem, qs, qr, ds, dr, as_, ar, bs, br):
    batch, toks, heads, npos, group = sizes
    chips = group // CORES
    rows = toks * heads
    half = GO // 2
    n_q, n_o = batch // GQ, batch // GO
    me = lax.axis_index('dcp')
    c, k = me // CORES, me % CORES
    ok = 1 - k
    cr, cl, cf = (c + 1) % chips, (c + chips - 1) % chips, (c + 2) % chips
    right, left, partner = cr * CORES + k, cl * CORES + k, c * CORES + ok

    barrier = pltpu.get_barrier_semaphore()
    for other in (right, left, partner):
        pl.semaphore_signal(barrier, inc=1, device_id={'dcp': other}, device_id_type=pl.DeviceIdType.MESH)

    def rcopy(src, dst, send, recv, dev):
        return pltpu.make_async_remote_copy(src_ref=src, dst_ref=dst, send_sem=send, recv_sem=recv,
                                            device_id={'dcp': dev}, device_id_type=pl.DeviceIdType.MESH)

    spans = ((0, AHEAD * GQ), (AHEAD * GQ, batch))

    def q_loads(n):
        span = slice(*spans[n])
        lat = [pltpu.make_async_copy(q_hbm.at[span, t, :, 0:LATENT], qall.at[k, c, span, :, t * LATENT:(t + 1) * LATENT], load_sem.at[n, t])
               for t in range(toks)]
        return lat, pltpu.make_async_copy(q_hbm.at[span, :, :, LATENT:LATENT + ROPE], rope_in.at[span], load_sem.at[n, toks])

    def q_ready(n):
        lat, rope = q_loads(n)
        span = slice(*spans[n])
        rope.wait()
        qall[k, c, span, :, toks * LATENT:] = jnp.concatenate([rope_in[span, t] for t in range(toks)], axis=-1)
        for cp in lat:
            cp.wait()

    def start(copies):
        for cp in copies:
            cp.start()

    for n in range(2):
        lat, rope = q_loads(n)
        start([rope] + lat)

    def kv_copy(b):
        slot = lax.rem(b, KV_SLOTS)
        return pltpu.make_async_copy(kv_hbm.at[b], kvb.at[slot], kv_sem.at[slot])

    def qreg(kk, cc, b0, n):
        return qall.at[kk, cc, pl.ds(b0, n)]

    def q_own(j):
        r = qreg(k, c, j * GQ, GQ)
        return [rcopy(r, r, qs.at[0, j], qr.at[0, j], right), rcopy(r, r, qs.at[1, j], qr.at[1, j], left),
                rcopy(r, r, qs.at[2, j], qr.at[2, j], partner)]

    def q_relay(j):
        lr, rr = qreg(k, cl, j * GQ, GQ), qreg(k, cr, j * GQ, GQ)
        lh, rh = qreg(k, cl, j * GQ, GQ // 2), qreg(k, cr, j * GQ + GQ // 2, GQ // 2)
        return [rcopy(lh, lh, qs.at[3, j], qr.at[3, j], right), rcopy(rh, rh, qs.at[4, j], qr.at[4, j], left),
                rcopy(lr, lr, qs.at[5, j], qr.at[5, j], partner), rcopy(rr, rr, qs.at[6, j], qr.at[6, j], partner)]

    def q_far(j):
        f0, f1 = qreg(k, cf, j * GQ, GQ // 2), qreg(k, cf, j * GQ + GQ // 2, GQ // 2)
        return [rcopy(f0, f0, qs.at[7, j], qr.at[7, j], partner), rcopy(f1, f1, qs.at[8, j], qr.at[8, j], partner)]

    def q_arrival(kind, j):
        full, h0, h1 = (j * GQ, GQ), (j * GQ, GQ // 2), (j * GQ + GQ // 2, GQ // 2)
        kk, cc, span = [(k, cl, full), (k, cr, full), (ok, c, full), (k, cf, h0), (k, cf, h1),
                        (ok, cl, full), (ok, cr, full), (ok, cf, h0), (ok, cf, h1)][kind]
        r = qreg(kk, cc, *span)
        return rcopy(r, r, qs.at[kind, j], qr.at[kind, j], partner)

    row_tok = (lax.broadcasted_iota(jnp.int32, (CORES * chips * rows, 1), 0) // heads) % toks
    key = lax.broadcasted_iota(jnp.int32, (1, npos), 1)
    pos = ((key // PAGE) * group + me) * PAGE + key % PAGE
    lanes = half * rows
    shift = lax.broadcasted_iota(jnp.int32, (chips * rows, lanes), 1) - lax.broadcasted_iota(jnp.int32, (chips * rows, lanes), 0) % rows
    lane_seq = lax.broadcasted_iota(jnp.int32, (chips, lanes), 1) // rows

    def scores(b):
        slot = lax.rem(b, KV_SLOTS)
        q = qall[:, :, b].reshape(CORES * chips, heads, toks * (LATENT + ROPE))
        lat = jnp.stack([q[:, :, t * LATENT:(t + 1) * LATENT] for t in range(toks)], axis=1).reshape(-1, LATENT)
        rope0 = toks * LATENT
        rope = jnp.stack([q[:, :, rope0 + t * ROPE:rope0 + (t + 1) * ROPE] for t in range(toks)], axis=1).reshape(-1, ROPE)
        q_rows = jnp.concatenate([lat, rope], axis=-1)
        return lax.dot_general(q_rows, kvb[slot], (((1,), (1,)), ((), ())), preferred_element_type=jnp.float32)

    def weights(b, s):
        s = jnp.where(pos <= len_ref[b] - toks + row_tok, s, -jnp.inf)
        m = jnp.max(s, axis=-1, keepdims=True)
        p = jnp.exp2((s - m) * SCALE2)
        return m, jnp.sum(p, axis=-1, keepdims=True), p.astype(jnp.bfloat16)

    def output(b, m, l, p):
        slot = lax.rem(b, KV_SLOTS)
        o = jnp.dot(p, kvb[slot, :, 0:LATENT], preferred_element_type=jnp.float32)
        o = (o * (1.0 / l)).astype(jnp.bfloat16)
        o_all[:, :, b] = o.reshape(CORES, chips, rows, LATENT)
        lse = m * SCALE2 + jnp.log2(l)
        place, in_half = b // half, b % half
        for kk in range(CORES):
            col = lse[kk * chips * rows:(kk + 1) * chips * rows]
            spread = jnp.where(shift == in_half * rows, col, 0.0).reshape(chips, rows, lanes)
            lse_all[kk, place] = jnp.where(lane_seq == in_half, jnp.sum(spread, axis=1), lse_all[kk, place])

    def attend(b0):
        bs_ = [b0 + u for u in range(UNROLL)]
        for b in bs_:
            kv_copy(b).wait()
        s = scores(bs_[0])
        for b in bs_:
            following = scores(b + 1) if b is not bs_[-1] else None
            output(b, *weights(b, s))
            s = following
        for b in bs_:
            @pl.when(b + KV_SLOTS < batch)
            def _():
                kv_copy(b + KV_SLOTS).start()

    def seqs(i, n=GO):
        return pl.ds(pl.multiple_of(i * n, n), n)

    def halves(i):
        return pl.ds(pl.multiple_of(2 * i, 2), 2)

    def columns(rows_):
        n = sum(r.shape[0] for r in rows_)
        return jnp.transpose(jnp.concatenate(rows_ + [jnp.zeros((8 - n, lanes), jnp.float32)] if n < 8 else rows_, axis=0))

    def merged(parts):
        top = functools.reduce(jnp.maximum, parts)
        total = top + jnp.log2(sum(jnp.exp2(x - top) for x in parts))
        return total, [jnp.exp2(x - total) for x in parts]

    def d_send(i):
        return [rcopy(o_all.at[ok, :, seqs(i)], prx.at[:, seqs(i)], ds.at[0, i], dr.at[0, i], partner),
                rcopy(lse_all.at[ok, halves(i)], plse.at[halves(i)], ds.at[1, i], dr.at[1, i], partner)]

    def d_merge(i):
        for cp in d_send(i):
            cp.wait_recv()
        w = []
        for h in range(2):
            total, (wa, wb) = merged([lse_all[k, 2 * i + h], plse[2 * i + h]])
            clse[2 * i + h] = total
            asnd[h, i] = clse[2 * i + h, pl.ds(cf, 1)]
            w.append(columns([wa, wb]))
        for j in range(GO):
            h, span = j // half, slice(j % half * rows, (j % half + 1) * rows)
            for cc in range(chips):
                x = o_all[k, cc, i * GO + j].astype(jnp.float32) * w[h][span, cc:cc + 1]
                y = prx[cc, i * GO + j].astype(jnp.float32) * w[h][span, chips + cc:chips + cc + 1]
                o_all[k, cc, i * GO + j] = (x + y).astype(jnp.bfloat16)

    def oreg(cc, i, part):
        if part is None:
            return o_all.at[k, cc, seqs(i)]
        return o_all.at[k, cc, pl.ds(i * GO + part * half, half)]

    def breg(side, i, part):
        return bbuf.at[side, pl.ds(i * GO + part * half, half)]

    def a_send(i):
        return [rcopy(oreg(cf, i, 0), abuf.at[0, pl.ds(i * half, half)], as_.at[0, i], ar.at[0, i], right),
                rcopy(oreg(cf, i, 1), abuf.at[1, pl.ds(i * half, half)], as_.at[1, i], ar.at[1, i], left),
                rcopy(asnd.at[0, i], alse.at[0, i], as_.at[2, i], ar.at[2, i], right),
                rcopy(asnd.at[1, i], alse.at[1, i], as_.at[3, i], ar.at[3, i], left)]

    def b_early(i):
        return [rcopy(oreg(cr, i, 1), breg(0, i, 1), bs.at[0, i], br.at[0, i], right),
                rcopy(oreg(cl, i, 0), breg(1, i, 0), bs.at[1, i], br.at[1, i], left)]

    def b_late(i):
        return [rcopy(oreg(cr, i, 0), breg(0, i, 0), bs.at[2, i], br.at[2, i], right),
                rcopy(oreg(cl, i, 1), breg(1, i, 1), bs.at[3, i], br.at[3, i], left),
                rcopy(bsnd.at[0, i], blse.at[0, i], bs.at[4, i], br.at[4, i], right),
                rcopy(bsnd.at[1, i], blse.at[1, i], bs.at[5, i], br.at[5, i], left)]

    def a_merge(i):
        for cp in a_send(i):
            cp.wait_recv()
        w, fresh = [], []
        for side, cc in ((0, cr), (1, cl)):
            total, both = merged([clse[2 * i + side, pl.ds(cc, 1)], alse[side, i]])
            fresh.append(total)
            w += both
        bsnd[0, i] = jnp.concatenate([fresh[0], clse[2 * i + 1, pl.ds(cr, 1)]], axis=0)
        bsnd[1, i] = jnp.concatenate([clse[2 * i, pl.ds(cl, 1)], fresh[1]], axis=0)
        w = columns(w)
        for side, cc in ((0, cr), (1, cl)):
            for j in range(half):
                b, span = i * GO + side * half + j, slice(j * rows, (j + 1) * rows)
                x = o_all[k, cc, b].astype(jnp.float32) * w[span, 2 * side:2 * side + 1]
                y = abuf[side, i * half + j].astype(jnp.float32) * w[span, 2 * side + 1:2 * side + 2]
                o_all[k, cc, b] = (x + y).astype(jnp.bfloat16)
        start(b_late(i))

    def final_merge(i):
        for cp in b_early(i) + b_late(i):
            cp.wait_recv()
        sent(b_late(i))
        own = jnp.concatenate([clse[2 * i + h, pl.ds(c, 1)] for h in range(2)], axis=0)
        w = columns(merged([own, blse[0, i], blse[1, i]])[1])
        for j in range(GO):
            b, h, span = i * GO + j, j // half, slice(j % half * rows, (j % half + 1) * rows)
            x = o_all[k, c, b].astype(jnp.float32) * w[span, h:h + 1]
            x += bbuf[0, b].astype(jnp.float32) * w[span, 2 + h:3 + h]
            x += bbuf[1, b].astype(jnp.float32) * w[span, 4 + h:5 + h]
            out_ref[b] = x.astype(jnp.bfloat16)

    def sent(copies):
        for cp in copies:
            cp.wait_send()

    def ring_start(lo, hi):
        lax.fori_loop(lo, hi, lambda i, carry: (start(a_send(i) + b_early(i)), carry)[1], 0)

    q_ready(0)
    pl.semaphore_wait(barrier, 3)
    for j in range(AHEAD):
        start(q_own(j))
    for b in range(KV_SLOTS):
        kv_copy(b).start()
    q_ready(1)

    def step(j, carry):
        @pl.when(j < n_q)
        def _():
            q_arrival(0, j).wait_recv()
            q_arrival(1, j).wait_recv()
            for cp in q_relay(j):
                cp.start()

        @pl.when(j + AHEAD < n_q)
        def _():
            for cp in q_own(j + AHEAD):
                cp.start()

        @pl.when((j >= 1) & (j <= n_q))
        def _():
            q_arrival(3, j - 1).wait_recv()
            q_arrival(4, j - 1).wait_recv()
            for cp in q_far(j - 1):
                cp.start()

        for at, op in enumerate((lambda: start(a_send(0)), lambda: start(b_early(0)), lambda: ring_start(1, 2), lambda: ring_start(2, n_o // 2),
                                 lambda: ring_start(n_o // 2, n_o - 2), lambda: ring_start(n_o - 2, n_o - 1))):
            pl.when(j == n_q - 4 + at)(op)

        @pl.when(j >= 2)
        def _():
            s = j - 2
            for kind in (2, 5, 6, 7, 8):
                q_arrival(kind, s).wait_recv()
            lax.fori_loop(0, GQ // UNROLL, lambda n, cc: (attend(s * GQ + n * UNROLL), cc)[1], 0)
            i = s // 2

            @pl.when(s % 2 == 1)
            def _():
                for cp in d_send(i):
                    cp.start()

            @pl.when((s % 2 == 0) & (s > 0))
            def _():
                d_merge(i - 1)

        return carry

    lax.fori_loop(0, n_q + 2, step, 0)
    d_merge(n_o - 1)
    ring_start(n_o - 1, n_o)
    lax.fori_loop(0, n_q, lambda j, cc: (sent(q_own(j) + q_relay(j) + q_far(j)), cc)[1], 0)
    lax.fori_loop(0, n_o, lambda i, cc: (a_merge(i), cc)[1], 0)
    lax.fori_loop(0, n_o, lambda i, cc: (sent(d_send(i) + a_send(i) + b_early(i)), cc)[1], 0)
    lax.fori_loop(0, n_o, lambda i, cc: (final_merge(i), cc)[1], 0)


def solution(mesh):
    group = mesh.shape['dcp']
    chips = group // CORES

    def local_step(q_blk, kv_blk, len_blk):
        batch, toks, heads, width = q_blk.shape
        npos = kv_blk.shape[1] * kv_blk.shape[2] * kv_blk.shape[3]
        rows, lanes = toks * heads, GO // 2 * toks * heads
        n_q, n_o = batch // GQ, batch // GO
        bf16, f32, dma = jnp.bfloat16, jnp.float32, pltpu.SemaphoreType.DMA
        any_space = pl.BlockSpec(memory_space=pl.ANY)
        out = pl.pallas_call(
            functools.partial(_kernel, (batch, toks, heads, npos, group)),
            out_shape=pltpu.VMEM((batch, rows, LATENT), bf16),
            in_specs=[any_space, any_space, pl.BlockSpec(memory_space=pltpu.SMEM)],
            out_specs=pl.BlockSpec(memory_space=pltpu.VMEM),
            scratch_shapes=[
                pltpu.VMEM((CORES, chips, batch, heads, toks * width), bf16),
                pltpu.VMEM((batch, toks, heads, ROPE), bf16),
                pltpu.VMEM((KV_SLOTS, npos, width), bf16),
                pltpu.VMEM((CORES, chips, batch, rows, LATENT), bf16),
                pltpu.VMEM((chips, batch, rows, LATENT), bf16),
                pltpu.VMEM((2, batch // 2, rows, LATENT), bf16),
                pltpu.VMEM((2, batch, rows, LATENT), bf16),
                pltpu.VMEM((CORES, 2 * n_o, chips, lanes), f32),
                pltpu.VMEM((2 * n_o, chips, lanes), f32),
                pltpu.VMEM((2 * n_o, chips, lanes), f32),
                pltpu.VMEM((2, n_o, 1, lanes), f32),
                pltpu.VMEM((2, n_o, 1, lanes), f32),
                pltpu.VMEM((2, n_o, 2, lanes), f32),
                pltpu.VMEM((2, n_o, 2, lanes), f32),
                dma((2, toks + 1)), dma((KV_SLOTS,)),
                dma((9, n_q)), dma((9, n_q)),
                dma((2, n_o)), dma((2, n_o)),
                dma((4, n_o)), dma((4, n_o)),
                dma((6, n_o)), dma((6, n_o)),
            ],
            compiler_params=pltpu.CompilerParams(collective_id=0, has_side_effects=True, vmem_limit_bytes=63_000_000),
            name='mla_ring',
        )(q_blk, kv_blk.reshape(batch, npos, width), len_blk)
        return out.reshape(batch, toks, heads, LATENT)

    return jax.shard_map(local_step, mesh=mesh, in_specs=(P('dp', None, 'dcp', None), P('dp', None, 'dcp', None, None), P('dp')),
                         out_specs=P('dp', None, 'dcp', None), check_vma=False)
```

```python
import functools
import math

import jax
import jax.numpy as jnp
from jax import lax
from jax.experimental import pallas as pl
from jax.experimental.pallas import tpu as pltpu
from jax.sharding import PartitionSpec as P

LATENT = 512
ROPE = 64
NOPE = 128
PAGE = 64
CORES = 2
SCALE2 = (NOPE + ROPE) ** -0.5 * math.log2(math.e)

GQ = 4
GO = 8
KV_SLOTS = 4
UNROLL = 2
AHEAD = 3


def _kernel(sizes, q_hbm, kv_hbm, len_hbm, out_ref,
            len_ref, qall, rope_in, kvb, o_all, prx, abuf, bbuf,
            lse_all, plse, clse, asnd, alse, bsnd, blse,
            load_sem, len_sem, kv_sem, qs, qr, ds, dr, as_, ar, bs, br):
    batch, toks, heads, npos, group = sizes
    chips = group // CORES
    rows = toks * heads
    half = GO // 2
    n_q, n_o = batch // GQ, batch // GO
    me = lax.axis_index('dcp')
    c, k = me // CORES, me % CORES
    ok = 1 - k
    cr, cl, cf = (c + 1) % chips, (c + chips - 1) % chips, (c + 2) % chips
    right, left, partner = cr * CORES + k, cl * CORES + k, c * CORES + ok

    barrier = pltpu.get_barrier_semaphore()
    for other in (right, left, partner):
        pl.semaphore_signal(barrier, inc=1, device_id={'dcp': other}, device_id_type=pl.DeviceIdType.MESH)

    def rcopy(src, dst, send, recv, dev):
        return pltpu.make_async_remote_copy(src_ref=src, dst_ref=dst, send_sem=send, recv_sem=recv,
                                            device_id={'dcp': dev}, device_id_type=pl.DeviceIdType.MESH)

    spans = ((0, AHEAD * GQ), (AHEAD * GQ, batch))

    def q_loads(n):
        span = slice(*spans[n])
        lat = [pltpu.make_async_copy(q_hbm.at[span, t, :, 0:LATENT], qall.at[k, c, span, :, t * LATENT:(t + 1) * LATENT], load_sem.at[n, t])
               for t in range(toks)]
        return lat, pltpu.make_async_copy(q_hbm.at[span, :, :, LATENT:LATENT + ROPE], rope_in.at[span], load_sem.at[n, toks])

    def q_ready(n):
        lat, rope = q_loads(n)
        span = slice(*spans[n])
        rope.wait()
        qall[k, c, span, :, toks * LATENT:] = jnp.concatenate([rope_in[span, t] for t in range(toks)], axis=-1)
        for cp in lat:
            cp.wait()

    def start(copies):
        for cp in copies:
            cp.start()

    for n in range(2):
        lat, rope = q_loads(n)
        start([rope] + lat)
    lengths = pltpu.make_async_copy(len_hbm, len_ref, len_sem)
    lengths.start()

    def kv_copy(b):
        slot = lax.rem(b, KV_SLOTS)
        return pltpu.make_async_copy(kv_hbm.at[b], kvb.at[slot], kv_sem.at[slot])

    def qreg(kk, cc, b0, n):
        return qall.at[kk, cc, pl.ds(b0, n)]

    def q_own(j):
        r = qreg(k, c, j * GQ, GQ)
        return [rcopy(r, r, qs.at[0, j], qr.at[0, j], right), rcopy(r, r, qs.at[1, j], qr.at[1, j], left),
                rcopy(r, r, qs.at[2, j], qr.at[2, j], partner)]

    def q_relay(j):
        lr, rr = qreg(k, cl, j * GQ, GQ), qreg(k, cr, j * GQ, GQ)
        lh, rh = qreg(k, cl, j * GQ, GQ // 2), qreg(k, cr, j * GQ + GQ // 2, GQ // 2)
        return [rcopy(lh, lh, qs.at[3, j], qr.at[3, j], right), rcopy(rh, rh, qs.at[4, j], qr.at[4, j], left),
                rcopy(lr, lr, qs.at[5, j], qr.at[5, j], partner), rcopy(rr, rr, qs.at[6, j], qr.at[6, j], partner)]

    def q_far(j):
        f0, f1 = qreg(k, cf, j * GQ, GQ // 2), qreg(k, cf, j * GQ + GQ // 2, GQ // 2)
        return [rcopy(f0, f0, qs.at[7, j], qr.at[7, j], partner), rcopy(f1, f1, qs.at[8, j], qr.at[8, j], partner)]

    def q_arrival(kind, j):
        full, h0, h1 = (j * GQ, GQ), (j * GQ, GQ // 2), (j * GQ + GQ // 2, GQ // 2)
        kk, cc, span = [(k, cl, full), (k, cr, full), (ok, c, full), (k, cf, h0), (k, cf, h1),
                        (ok, cl, full), (ok, cr, full), (ok, cf, h0), (ok, cf, h1)][kind]
        r = qreg(kk, cc, *span)
        return rcopy(r, r, qs.at[kind, j], qr.at[kind, j], partner)

    row_tok = (lax.broadcasted_iota(jnp.int32, (CORES * chips * rows, 1), 0) // heads) % toks
    key = lax.broadcasted_iota(jnp.int32, (1, npos), 1)
    pos = ((key // PAGE) * group + me) * PAGE + key % PAGE
    lanes = half * rows
    shift = lax.broadcasted_iota(jnp.int32, (chips * rows, lanes), 1) - lax.broadcasted_iota(jnp.int32, (chips * rows, lanes), 0) % rows
    lane_seq = lax.broadcasted_iota(jnp.int32, (chips, lanes), 1) // rows

    def scores(b):
        slot = lax.rem(b, KV_SLOTS)
        q = qall[:, :, b].reshape(CORES * chips, heads, toks * (LATENT + ROPE))
        lat = jnp.stack([q[:, :, t * LATENT:(t + 1) * LATENT] for t in range(toks)], axis=1).reshape(-1, LATENT)
        rope0 = toks * LATENT
        rope = jnp.stack([q[:, :, rope0 + t * ROPE:rope0 + (t + 1) * ROPE] for t in range(toks)], axis=1).reshape(-1, ROPE)
        q_rows = jnp.concatenate([lat, rope], axis=-1)
        return lax.dot_general(q_rows, kvb[slot], (((1,), (1,)), ((), ())), preferred_element_type=jnp.float32)

    def weights(b, s):
        s = jnp.where(pos <= len_ref[b] - toks + row_tok, s, -jnp.inf)
        m = jnp.max(s, axis=-1, keepdims=True)
        p = jnp.exp2((s - m) * SCALE2)
        return m, jnp.sum(p, axis=-1, keepdims=True), p.astype(jnp.bfloat16)

    def output(b, m, l, p):
        slot = lax.rem(b, KV_SLOTS)
        o = jnp.dot(p, kvb[slot, :, 0:LATENT], preferred_element_type=jnp.float32)
        o = (o * (1.0 / l)).astype(jnp.bfloat16)
        o_all[:, :, b] = o.reshape(CORES, chips, rows, LATENT)
        lse = m * SCALE2 + jnp.log2(l)
        place, in_half = b // half, b % half
        for kk in range(CORES):
            col = lse[kk * chips * rows:(kk + 1) * chips * rows]
            spread = jnp.where(shift == in_half * rows, col, 0.0).reshape(chips, rows, lanes)
            lse_all[kk, place] = jnp.where(lane_seq == in_half, jnp.sum(spread, axis=1), lse_all[kk, place])

    def attend(b0):
        bs_ = [b0 + u for u in range(UNROLL)]
        for b in bs_:
            kv_copy(b).wait()
        s = scores(bs_[0])
        for b in bs_:
            following = scores(b + 1) if b is not bs_[-1] else None
            output(b, *weights(b, s))
            s = following
        for b in bs_:
            @pl.when(b + KV_SLOTS < batch)
            def _():
                kv_copy(b + KV_SLOTS).start()

    def seqs(i, n=GO):
        return pl.ds(pl.multiple_of(i * n, n), n)

    def halves(i):
        return pl.ds(pl.multiple_of(2 * i, 2), 2)

    def columns(rows_):
        n = sum(r.shape[0] for r in rows_)
        return jnp.transpose(jnp.concatenate(rows_ + [jnp.zeros((8 - n, lanes), jnp.float32)] if n < 8 else rows_, axis=0))

    def merged(parts):
        top = functools.reduce(jnp.maximum, parts)
        total = top + jnp.log2(sum(jnp.exp2(x - top) for x in parts))
        return total, [jnp.exp2(x - total) for x in parts]

    def d_send(i):
        return [rcopy(o_all.at[ok, :, seqs(i)], prx.at[:, seqs(i)], ds.at[0, i], dr.at[0, i], partner),
                rcopy(lse_all.at[ok, halves(i)], plse.at[halves(i)], ds.at[1, i], dr.at[1, i], partner)]

    def d_merge(i):
        for cp in d_send(i):
            cp.wait_recv()
        w = []
        for h in range(2):
            total, (wa, wb) = merged([lse_all[k, 2 * i + h], plse[2 * i + h]])
            clse[2 * i + h] = total
            asnd[h, i] = clse[2 * i + h, pl.ds(cf, 1)]
            w.append(columns([wa, wb]))
        for j in range(GO):
            h, span = j // half, slice(j % half * rows, (j % half + 1) * rows)
            for cc in range(chips):
                x = o_all[k, cc, i * GO + j].astype(jnp.float32) * w[h][span, cc:cc + 1]
                y = prx[cc, i * GO + j].astype(jnp.float32) * w[h][span, chips + cc:chips + cc + 1]
                o_all[k, cc, i * GO + j] = (x + y).astype(jnp.bfloat16)

    def oreg(cc, i, part):
        if part is None:
            return o_all.at[k, cc, seqs(i)]
        return o_all.at[k, cc, pl.ds(i * GO + part * half, half)]

    def breg(side, i, part):
        return bbuf.at[side, pl.ds(i * GO + part * half, half)]

    def a_send(i):
        return [rcopy(oreg(cf, i, 0), abuf.at[0, pl.ds(i * half, half)], as_.at[0, i], ar.at[0, i], right),
                rcopy(oreg(cf, i, 1), abuf.at[1, pl.ds(i * half, half)], as_.at[1, i], ar.at[1, i], left),
                rcopy(asnd.at[0, i], alse.at[0, i], as_.at[2, i], ar.at[2, i], right),
                rcopy(asnd.at[1, i], alse.at[1, i], as_.at[3, i], ar.at[3, i], left)]

    def b_early(i):
        return [rcopy(oreg(cr, i, 1), breg(0, i, 1), bs.at[0, i], br.at[0, i], right),
                rcopy(oreg(cl, i, 0), breg(1, i, 0), bs.at[1, i], br.at[1, i], left)]

    def b_late(i):
        return [rcopy(bsnd.at[0, i], blse.at[0, i], bs.at[4, i], br.at[4, i], right),
                rcopy(bsnd.at[1, i], blse.at[1, i], bs.at[5, i], br.at[5, i], left),
                rcopy(oreg(cr, i, 0), breg(0, i, 0), bs.at[2, i], br.at[2, i], right),
                rcopy(oreg(cl, i, 1), breg(1, i, 1), bs.at[3, i], br.at[3, i], left)]

    def a_merge(i):
        for cp in a_send(i):
            cp.wait_recv()
        w, fresh = [], []
        for side, cc in ((0, cr), (1, cl)):
            total, both = merged([clse[2 * i + side, pl.ds(cc, 1)], alse[side, i]])
            fresh.append(total)
            w += both
        bsnd[0, i] = jnp.concatenate([fresh[0], clse[2 * i + 1, pl.ds(cr, 1)]], axis=0)
        bsnd[1, i] = jnp.concatenate([clse[2 * i, pl.ds(cl, 1)], fresh[1]], axis=0)
        w = columns(w)
        for side, cc in ((0, cr), (1, cl)):
            for j in range(half):
                b, span = i * GO + side * half + j, slice(j * rows, (j + 1) * rows)
                x = o_all[k, cc, b].astype(jnp.float32) * w[span, 2 * side:2 * side + 1]
                y = abuf[side, i * half + j].astype(jnp.float32) * w[span, 2 * side + 1:2 * side + 2]
                o_all[k, cc, b] = (x + y).astype(jnp.bfloat16)
        start(b_late(i))

    def final_merge(i):
        late = b_late(i)
        for cp in b_early(i) + late[:2]:
            cp.wait_recv()
        own = jnp.concatenate([clse[2 * i + h, pl.ds(c, 1)] for h in range(2)], axis=0)
        w = columns(merged([own, blse[0, i], blse[1, i]])[1])
        for h in range(2):
            late[2 + h].wait_recv()
            for j in range(half):
                b, span = i * GO + h * half + j, slice(j * rows, (j + 1) * rows)
                x = o_all[k, c, b].astype(jnp.float32) * w[span, h:h + 1]
                x += bbuf[0, b].astype(jnp.float32) * w[span, 2 + h:3 + h]
                x += bbuf[1, b].astype(jnp.float32) * w[span, 4 + h:5 + h]
                out_ref[b] = x.astype(jnp.bfloat16)
        sent(late)

    def sent(copies):
        for cp in copies:
            cp.wait_send()

    def ring_start(lo, hi):
        lax.fori_loop(lo, hi, lambda i, carry: (start(a_send(i) + b_early(i)), carry)[1], 0)

    q_ready(0)
    pl.semaphore_wait(barrier, 3)
    for j in range(AHEAD):
        start(q_own(j))
    for b in range(KV_SLOTS):
        kv_copy(b).start()
    q_ready(1)
    lengths.wait()

    def step(j, carry):
        @pl.when(j < n_q)
        def _():
            q_arrival(0, j).wait_recv()
            q_arrival(1, j).wait_recv()
            for cp in q_relay(j):
                cp.start()

        @pl.when(j + AHEAD < n_q)
        def _():
            for cp in q_own(j + AHEAD):
                cp.start()

        @pl.when((j >= 1) & (j <= n_q))
        def _():
            q_arrival(3, j - 1).wait_recv()
            q_arrival(4, j - 1).wait_recv()
            for cp in q_far(j - 1):
                cp.start()

        for at, op in enumerate((lambda: start(a_send(0)), lambda: start(b_early(0)), lambda: ring_start(1, 2), lambda: ring_start(2, n_o // 2),
                                 lambda: ring_start(n_o // 2, n_o - 2), lambda: ring_start(n_o - 2, n_o - 1))):
            pl.when(j == n_q - 4 + at)(op)

        @pl.when(j >= 2)
        def _():
            s = j - 2
            for kind in (2, 5, 6, 7, 8):
                q_arrival(kind, s).wait_recv()
            lax.fori_loop(0, GQ // UNROLL, lambda n, cc: (attend(s * GQ + n * UNROLL), cc)[1], 0)
            i = s // 2

            @pl.when(s % 2 == 1)
            def _():
                for cp in d_send(i):
                    cp.start()

            @pl.when((s % 2 == 0) & (s > 0))
            def _():
                d_merge(i - 1)

        return carry

    lax.fori_loop(0, n_q + 2, step, 0)
    d_merge(n_o - 1)
    ring_start(n_o - 1, n_o)
    lax.fori_loop(0, n_q, lambda j, cc: (sent(q_own(j) + q_relay(j) + q_far(j)), cc)[1], 0)
    lax.fori_loop(0, n_o, lambda i, cc: (a_merge(i), cc)[1], 0)
    lax.fori_loop(0, n_o, lambda i, cc: (sent(d_send(i) + a_send(i) + b_early(i)), cc)[1], 0)
    lax.fori_loop(0, n_o, lambda i, cc: (final_merge(i), cc)[1], 0)


def solution(mesh):
    group = mesh.shape['dcp']
    chips = group // CORES

    def local_step(q_blk, kv_blk, len_blk):
        batch, toks, heads, width = q_blk.shape
        npos = kv_blk.shape[1] * kv_blk.shape[2] * kv_blk.shape[3]
        rows, lanes = toks * heads, GO // 2 * toks * heads
        n_q, n_o = batch // GQ, batch // GO
        bf16, f32, dma = jnp.bfloat16, jnp.float32, pltpu.SemaphoreType.DMA
        any_space = pl.BlockSpec(memory_space=pl.ANY)
        out = pl.pallas_call(
            functools.partial(_kernel, (batch, toks, heads, npos, group)),
            out_shape=pltpu.VMEM((batch, rows, LATENT), bf16),
            in_specs=[any_space, any_space, any_space],
            out_specs=pl.BlockSpec(memory_space=pltpu.VMEM),
            scratch_shapes=[
                pltpu.SMEM((batch,), jnp.int32),
                pltpu.VMEM((CORES, chips, batch, heads, toks * width), bf16),
                pltpu.VMEM((batch, toks, heads, ROPE), bf16),
                pltpu.VMEM((KV_SLOTS, npos, width), bf16),
                pltpu.VMEM((CORES, chips, batch, rows, LATENT), bf16),
                pltpu.VMEM((chips, batch, rows, LATENT), bf16),
                pltpu.VMEM((2, batch // 2, rows, LATENT), bf16),
                pltpu.VMEM((2, batch, rows, LATENT), bf16),
                pltpu.VMEM((CORES, 2 * n_o, chips, lanes), f32),
                pltpu.VMEM((2 * n_o, chips, lanes), f32),
                pltpu.VMEM((2 * n_o, chips, lanes), f32),
                pltpu.VMEM((2, n_o, 1, lanes), f32),
                pltpu.VMEM((2, n_o, 1, lanes), f32),
                pltpu.VMEM((2, n_o, 2, lanes), f32),
                pltpu.VMEM((2, n_o, 2, lanes), f32),
                dma((2, toks + 1)), dma, dma((KV_SLOTS,)),
                dma((9, n_q)), dma((9, n_q)),
                dma((2, n_o)), dma((2, n_o)),
                dma((4, n_o)), dma((4, n_o)),
                dma((6, n_o)), dma((6, n_o)),
            ],
            compiler_params=pltpu.CompilerParams(collective_id=0, has_side_effects=True, vmem_limit_bytes=63_000_000),
            name='mla_ring',
        )(q_blk, kv_blk.reshape(batch, npos, width), len_blk)
        return out.reshape(batch, toks, heads, LATENT)

    return jax.shard_map(local_step, mesh=mesh, in_specs=(P('dp', None, 'dcp', None), P('dp', None, 'dcp', None, None), P('dp')),
                         out_specs=P('dp', None, 'dcp', None), check_vma=False)
```

```python
import functools
import math

import jax
import jax.numpy as jnp
from jax import lax
from jax.experimental import pallas as pl
from jax.experimental.pallas import tpu as pltpu
from jax.sharding import PartitionSpec as P

LATENT = 512
ROPE = 64
NOPE = 128
PAGE = 64
CORES = 2
SCALE2 = (NOPE + ROPE) ** -0.5 * math.log2(math.e)

GQ = 4
GO = 8
KV_SLOTS = 4
UNROLL = 2
AHEAD = 3


def _kernel(sizes, q_hbm, kv_hbm, len_hbm, out_ref,
            len_ref, qall, rope_in, kvb, o_all, prx, abuf, bbuf,
            lse_all, plse, clse, asnd, alse, bsnd, blse,
            turn, load_sem, len_sem, kv_sem, qs, qr, ds, dr, as_, ar, bs, br):
    batch, toks, heads, npos, group = sizes
    chips = group // CORES
    rows = toks * heads
    half = GO // 2
    n_q, n_o = batch // GQ, batch // GO
    me = lax.axis_index('dcp')
    c, k = me // CORES, me % CORES
    ok = 1 - k
    cr, cl, cf = (c + 1) % chips, (c + chips - 1) % chips, (c + 2) % chips
    right, left, partner = cr * CORES + k, cl * CORES + k, c * CORES + ok

    barrier = pltpu.get_barrier_semaphore()
    for other in (right, left, partner):
        pl.semaphore_signal(barrier, inc=1, device_id={'dcp': other}, device_id_type=pl.DeviceIdType.MESH)

    def rcopy(src, dst, send, recv, dev):
        return pltpu.make_async_remote_copy(src_ref=src, dst_ref=dst, send_sem=send, recv_sem=recv,
                                            device_id={'dcp': dev}, device_id_type=pl.DeviceIdType.MESH)

    spans = ((0, AHEAD * GQ), (AHEAD * GQ, batch))

    def q_loads(n):
        span = slice(*spans[n])
        lat = [pltpu.make_async_copy(q_hbm.at[span, t, :, 0:LATENT], qall.at[k, c, span, :, t * LATENT:(t + 1) * LATENT], load_sem.at[n, t])
               for t in range(toks)]
        return lat, pltpu.make_async_copy(q_hbm.at[span, :, :, LATENT:LATENT + ROPE], rope_in.at[span], load_sem.at[n, toks])

    def q_ready(n):
        lat, rope = q_loads(n)
        span = slice(*spans[n])
        rope.wait()
        qall[k, c, span, :, toks * LATENT:] = jnp.concatenate([rope_in[span, t] for t in range(toks)], axis=-1)
        for cp in lat:
            cp.wait()

    def start(copies):
        for cp in copies:
            cp.start()

    for n in range(2):
        lat, rope = q_loads(n)
        start([rope] + lat)
    lengths = pltpu.make_async_copy(len_hbm, len_ref, len_sem)
    lengths.start()

    def kv_copy(b):
        slot = lax.rem(b, KV_SLOTS)
        return pltpu.make_async_copy(kv_hbm.at[b], kvb.at[slot], kv_sem.at[slot])

    def qreg(kk, cc, b0, n):
        return qall.at[kk, cc, pl.ds(b0, n)]

    def q_own(j):
        r = qreg(k, c, j * GQ, GQ)
        return [rcopy(r, r, qs.at[0, j], qr.at[0, j], right), rcopy(r, r, qs.at[1, j], qr.at[1, j], left),
                rcopy(r, r, qs.at[2, j], qr.at[2, j], partner)]

    def q_relay(j):
        lr, rr = qreg(k, cl, j * GQ, GQ), qreg(k, cr, j * GQ, GQ)
        lh, rh = qreg(k, cl, j * GQ, GQ // 2), qreg(k, cr, j * GQ + GQ // 2, GQ // 2)
        return [rcopy(lh, lh, qs.at[3, j], qr.at[3, j], right), rcopy(rh, rh, qs.at[4, j], qr.at[4, j], left),
                rcopy(lr, lr, qs.at[5, j], qr.at[5, j], partner), rcopy(rr, rr, qs.at[6, j], qr.at[6, j], partner)]

    def q_far(j):
        f0, f1 = qreg(k, cf, j * GQ, GQ // 2), qreg(k, cf, j * GQ + GQ // 2, GQ // 2)
        return [rcopy(f0, f0, qs.at[7, j], qr.at[7, j], partner), rcopy(f1, f1, qs.at[8, j], qr.at[8, j], partner)]

    def q_arrival(kind, j):
        full, h0, h1 = (j * GQ, GQ), (j * GQ, GQ // 2), (j * GQ + GQ // 2, GQ // 2)
        kk, cc, span = [(k, cl, full), (k, cr, full), (ok, c, full), (k, cf, h0), (k, cf, h1),
                        (ok, cl, full), (ok, cr, full), (ok, cf, h0), (ok, cf, h1)][kind]
        r = qreg(kk, cc, *span)
        return rcopy(r, r, qs.at[kind, j], qr.at[kind, j], partner)

    row_tok = (lax.broadcasted_iota(jnp.int32, (CORES * chips * rows, 1), 0) // heads) % toks
    key = lax.broadcasted_iota(jnp.int32, (1, npos), 1)
    pos = ((key // PAGE) * group + me) * PAGE + key % PAGE
    lanes = half * rows
    shift = lax.broadcasted_iota(jnp.int32, (chips * rows, lanes), 1) - lax.broadcasted_iota(jnp.int32, (chips * rows, lanes), 0) % rows
    lane_seq = lax.broadcasted_iota(jnp.int32, (chips, lanes), 1) // rows

    def scores(b):
        slot = lax.rem(b, KV_SLOTS)
        q = qall[:, :, b].reshape(CORES * chips, heads, toks * (LATENT + ROPE))
        lat = jnp.stack([q[:, :, t * LATENT:(t + 1) * LATENT] for t in range(toks)], axis=1).reshape(-1, LATENT)
        rope0 = toks * LATENT
        rope = jnp.stack([q[:, :, rope0 + t * ROPE:rope0 + (t + 1) * ROPE] for t in range(toks)], axis=1).reshape(-1, ROPE)
        q_rows = jnp.concatenate([lat, rope], axis=-1)
        return lax.dot_general(q_rows, kvb[slot], (((1,), (1,)), ((), ())), preferred_element_type=jnp.float32)

    def weights(b, s):
        s = jnp.where(pos <= len_ref[b] - toks + row_tok, s, -jnp.inf)
        m = jnp.max(s, axis=-1, keepdims=True)
        p = jnp.exp2((s - m) * SCALE2)
        return m, jnp.sum(p, axis=-1, keepdims=True), p.astype(jnp.bfloat16)

    def output(b, m, l, p):
        slot = lax.rem(b, KV_SLOTS)
        o = jnp.dot(p, kvb[slot, :, 0:LATENT], preferred_element_type=jnp.float32)
        o = (o * (1.0 / l)).astype(jnp.bfloat16)
        o_all[:, :, b] = o.reshape(CORES, chips, rows, LATENT)
        lse = m * SCALE2 + jnp.log2(l)
        place, in_half = b // half, b % half
        for kk in range(CORES):
            col = lse[kk * chips * rows:(kk + 1) * chips * rows]
            spread = jnp.where(shift == in_half * rows, col, 0.0).reshape(chips, rows, lanes)
            lse_all[kk, place] = jnp.where(lane_seq == in_half, jnp.sum(spread, axis=1), lse_all[kk, place])

    def attend(b0):
        bs_ = [b0 + u for u in range(UNROLL)]
        for b in bs_:
            kv_copy(b).wait()
        s = scores(bs_[0])
        for b in bs_:
            following = scores(b + 1) if b is not bs_[-1] else None
            output(b, *weights(b, s))
            s = following
        for b in bs_:
            @pl.when(b + KV_SLOTS < batch)
            def _():
                kv_copy(b + KV_SLOTS).start()

    def seqs(i, n=GO):
        return pl.ds(pl.multiple_of(i * n, n), n)

    def halves(i):
        return pl.ds(pl.multiple_of(2 * i, 2), 2)

    def columns(rows_):
        n = sum(r.shape[0] for r in rows_)
        return jnp.transpose(jnp.concatenate(rows_ + [jnp.zeros((8 - n, lanes), jnp.float32)] if n < 8 else rows_, axis=0))

    def merged(parts):
        top = functools.reduce(jnp.maximum, parts)
        total = top + jnp.log2(sum(jnp.exp2(x - top) for x in parts))
        return total, [jnp.exp2(x - total) for x in parts]

    def d_send(i):
        return [rcopy(o_all.at[ok, :, seqs(i)], prx.at[:, seqs(i)], ds.at[0, i], dr.at[0, i], partner),
                rcopy(lse_all.at[ok, halves(i)], plse.at[halves(i)], ds.at[1, i], dr.at[1, i], partner)]

    def d_merge(i):
        for cp in d_send(i):
            cp.wait_recv()
        w = []
        for h in range(2):
            total, (wa, wb) = merged([lse_all[k, 2 * i + h], plse[2 * i + h]])
            clse[2 * i + h] = total
            asnd[h, i] = clse[2 * i + h, pl.ds(cf, 1)]
            w.append(columns([wa, wb]))
        for j in range(GO):
            h, span = j // half, slice(j % half * rows, (j % half + 1) * rows)
            for cc in range(chips):
                x = o_all[k, cc, i * GO + j].astype(jnp.float32) * w[h][span, cc:cc + 1]
                y = prx[cc, i * GO + j].astype(jnp.float32) * w[h][span, chips + cc:chips + cc + 1]
                o_all[k, cc, i * GO + j] = (x + y).astype(jnp.bfloat16)

    def oreg(cc, i, part):
        if part is None:
            return o_all.at[k, cc, seqs(i)]
        return o_all.at[k, cc, pl.ds(i * GO + part * half, half)]

    def breg(side, i, part):
        return bbuf.at[side, pl.ds(i * GO + part * half, half)]

    def a_send(i):
        return [rcopy(oreg(cf, i, 0), abuf.at[0, pl.ds(i * half, half)], as_.at[0, i], ar.at[0, i], right),
                rcopy(oreg(cf, i, 1), abuf.at[1, pl.ds(i * half, half)], as_.at[1, i], ar.at[1, i], left),
                rcopy(asnd.at[0, i], alse.at[0, i], as_.at[2, i], ar.at[2, i], right),
                rcopy(asnd.at[1, i], alse.at[1, i], as_.at[3, i], ar.at[3, i], left)]

    def b_early(i):
        return [rcopy(oreg(cr, i, 1), breg(0, i, 1), bs.at[0, i], br.at[0, i], right),
                rcopy(oreg(cl, i, 0), breg(1, i, 0), bs.at[1, i], br.at[1, i], left)]

    def b_late(i):
        return [rcopy(bsnd.at[0, i], blse.at[0, i], bs.at[4, i], br.at[4, i], right),
                rcopy(bsnd.at[1, i], blse.at[1, i], bs.at[5, i], br.at[5, i], left),
                rcopy(oreg(cr, i, 0), breg(0, i, 0), bs.at[2, i], br.at[2, i], right),
                rcopy(oreg(cl, i, 1), breg(1, i, 1), bs.at[3, i], br.at[3, i], left)]

    def a_merge(i):
        for cp in a_send(i):
            cp.wait_recv()
        pl.when(i > 0)(lambda: start(b_late(i - 1)))
        w, fresh = [], []
        for side, cc in ((0, cr), (1, cl)):
            total, both = merged([clse[2 * i + side, pl.ds(cc, 1)], alse[side, i]])
            fresh.append(total)
            w += both
        bsnd[0, i] = jnp.concatenate([fresh[0], clse[2 * i + 1, pl.ds(cr, 1)]], axis=0)
        bsnd[1, i] = jnp.concatenate([clse[2 * i, pl.ds(cl, 1)], fresh[1]], axis=0)
        w = columns(w)
        for side, cc in ((0, cr), (1, cl)):
            for j in range(half):
                b, span = i * GO + side * half + j, slice(j * rows, (j + 1) * rows)
                x = o_all[k, cc, b].astype(jnp.float32) * w[span, 2 * side:2 * side + 1]
                y = abuf[side, i * half + j].astype(jnp.float32) * w[span, 2 * side + 1:2 * side + 2]
                o_all[k, cc, b] = (x + y).astype(jnp.bfloat16)

    def final_merge(i):
        late = b_late(i)
        for cp in b_early(i) + late[:2]:
            cp.wait_recv()
        own = jnp.concatenate([clse[2 * i + h, pl.ds(c, 1)] for h in range(2)], axis=0)
        w = columns(merged([own, blse[0, i], blse[1, i]])[1])
        for h in range(2):
            late[2 + h].wait_recv()
            for j in range(half):
                b, span = i * GO + h * half + j, slice(j * rows, (j + 1) * rows)
                x = o_all[k, c, b].astype(jnp.float32) * w[span, h:h + 1]
                x += bbuf[0, b].astype(jnp.float32) * w[span, 2 + h:3 + h]
                x += bbuf[1, b].astype(jnp.float32) * w[span, 4 + h:5 + h]
                out_ref[b] = x.astype(jnp.bfloat16)
        sent(late)

    def sent(copies):
        for cp in copies:
            cp.wait_send()

    def ring_start(lo, hi):
        lax.fori_loop(lo, hi, lambda i, carry: (start(a_send(i) + b_early(i)), carry)[1], 0)

    q_ready(0)
    pl.semaphore_wait(barrier, 3)
    pl.when(k == CORES - 1)(lambda: pl.semaphore_wait(turn, 1))
    for j in range(AHEAD):
        start(q_own(j))
    pl.when(k == 0)(lambda: pl.semaphore_signal(turn, inc=1, device_id={'dcp': partner}, device_id_type=pl.DeviceIdType.MESH))
    for b in range(KV_SLOTS):
        kv_copy(b).start()
    q_ready(1)
    lengths.wait()

    def step(j, carry):
        @pl.when(j < n_q)
        def _():
            q_arrival(0, j).wait_recv()
            q_arrival(1, j).wait_recv()
            for cp in q_relay(j):
                cp.start()

        @pl.when(j + AHEAD < n_q)
        def _():
            for cp in q_own(j + AHEAD):
                cp.start()

        @pl.when((j >= 1) & (j <= n_q))
        def _():
            q_arrival(3, j - 1).wait_recv()
            q_arrival(4, j - 1).wait_recv()
            for cp in q_far(j - 1):
                cp.start()

        for at, op in enumerate((lambda: start(a_send(0)), lambda: start(b_early(0)), lambda: ring_start(1, 2), lambda: ring_start(2, n_o // 2),
                                 lambda: ring_start(n_o // 2, n_o - 2), lambda: ring_start(n_o - 2, n_o - 1))):
            pl.when(j == n_q - 4 + at)(op)

        @pl.when((j >= 4) & (j % 2 == 0))
        def _():
            start(d_send(j // 2 - 2))

        @pl.when(j >= 2)
        def _():
            s = j - 2
            for kind in (2, 5, 6, 7, 8):
                q_arrival(kind, s).wait_recv()
            lax.fori_loop(0, GQ // UNROLL, lambda n, cc: (attend(s * GQ + n * UNROLL), cc)[1], 0)

            @pl.when((s % 2 == 0) & (s > 0))
            def _():
                d_merge(s // 2 - 1)

        return carry

    def each(lo, hi, op):
        lax.fori_loop(lo, hi, lambda i, carry: (op(i), carry)[1], 0)

    each(0, n_q + 2, lambda j: step(j, 0))
    each(0, n_q // 2, lambda j: sent(q_own(j) + q_relay(j) + q_far(j)))
    start(d_send(n_o - 1))
    d_merge(n_o - 1)
    each(n_q // 2, n_q, lambda j: sent(q_own(j) + q_relay(j) + q_far(j)))
    ring_start(n_o - 1, n_o)
    each(0, n_o, a_merge)
    each(0, n_o, lambda i: sent(d_send(i)))
    start(b_late(n_o - 1))
    each(0, n_o, lambda i: sent(a_send(i) + b_early(i)))
    each(0, n_o, final_merge)


def solution(mesh):
    group = mesh.shape['dcp']
    chips = group // CORES

    def local_step(q_blk, kv_blk, len_blk):
        batch, toks, heads, width = q_blk.shape
        npos = kv_blk.shape[1] * kv_blk.shape[2] * kv_blk.shape[3]
        rows, lanes = toks * heads, GO // 2 * toks * heads
        n_q, n_o = batch // GQ, batch // GO
        bf16, f32, dma = jnp.bfloat16, jnp.float32, pltpu.SemaphoreType.DMA
        any_space = pl.BlockSpec(memory_space=pl.ANY)
        out = pl.pallas_call(
            functools.partial(_kernel, (batch, toks, heads, npos, group)),
            out_shape=pltpu.VMEM((batch, rows, LATENT), bf16),
            in_specs=[any_space, any_space, any_space],
            out_specs=pl.BlockSpec(memory_space=pltpu.VMEM),
            scratch_shapes=[
                pltpu.SMEM((batch,), jnp.int32),
                pltpu.VMEM((CORES, chips, batch, heads, toks * width), bf16),
                pltpu.VMEM((batch, toks, heads, ROPE), bf16),
                pltpu.VMEM((KV_SLOTS, npos, width), bf16),
                pltpu.VMEM((CORES, chips, batch, rows, LATENT), bf16),
                pltpu.VMEM((chips, batch, rows, LATENT), bf16),
                pltpu.VMEM((2, batch // 2, rows, LATENT), bf16),
                pltpu.VMEM((2, batch, rows, LATENT), bf16),
                pltpu.VMEM((CORES, 2 * n_o, chips, lanes), f32),
                pltpu.VMEM((2 * n_o, chips, lanes), f32),
                pltpu.VMEM((2 * n_o, chips, lanes), f32),
                pltpu.VMEM((2, n_o, 1, lanes), f32),
                pltpu.VMEM((2, n_o, 1, lanes), f32),
                pltpu.VMEM((2, n_o, 2, lanes), f32),
                pltpu.VMEM((2, n_o, 2, lanes), f32),
                pltpu.SemaphoreType.REGULAR, dma((2, toks + 1)), dma, dma((KV_SLOTS,)),
                dma((9, n_q)), dma((9, n_q)),
                dma((2, n_o)), dma((2, n_o)),
                dma((4, n_o)), dma((4, n_o)),
                dma((6, n_o)), dma((6, n_o)),
            ],
            compiler_params=pltpu.CompilerParams(collective_id=0, has_side_effects=True, vmem_limit_bytes=63_000_000),
            name='mla_ring',
        )(q_blk, kv_blk.reshape(batch, npos, width), len_blk)
        return out.reshape(batch, toks, heads, LATENT)

    return jax.shard_map(local_step, mesh=mesh, in_specs=(P('dp', None, 'dcp', None), P('dp', None, 'dcp', None, None), P('dp')),
                         out_specs=P('dp', None, 'dcp', None), check_vma=False)
```

```python
import functools
import math

import jax
import jax.numpy as jnp
from jax import lax
from jax.experimental import pallas as pl
from jax.experimental.pallas import tpu as pltpu
from jax.sharding import PartitionSpec as P

LATENT = 512
ROPE = 64
NOPE = 128
PAGE = 64
CORES = 2
SCALE2 = (NOPE + ROPE) ** -0.5 * math.log2(math.e)

GQ = 4
GO = 8
KV_SLOTS = 4
UNROLL = 2
AHEAD = 3


def _kernel(sizes, q_hbm, kv_hbm, len_hbm, out_ref,
            len_ref, qall, rope_in, kvb, o_all, prx, abuf, bbuf,
            lse_all, plse, clse, asnd, alse, bsnd, blse,
            load_sem, len_sem, kv_sem, qs, qr, ds, dr, as_, ar, bs, br):
    batch, toks, heads, npos, group = sizes
    chips = group // CORES
    rows = toks * heads
    half = GO // 2
    n_q, n_o = batch // GQ, batch // GO
    me = lax.axis_index('dcp')
    c, k = me // CORES, me % CORES
    ok = 1 - k
    cr, cl, cf = (c + 1) % chips, (c + chips - 1) % chips, (c + 2) % chips
    right, left, partner = cr * CORES + k, cl * CORES + k, c * CORES + ok

    barrier = pltpu.get_barrier_semaphore()
    for other in (right, left, partner):
        pl.semaphore_signal(barrier, inc=1, device_id={'dcp': other}, device_id_type=pl.DeviceIdType.MESH)

    def rcopy(src, dst, send, recv, dev):
        return pltpu.make_async_remote_copy(src_ref=src, dst_ref=dst, send_sem=send, recv_sem=recv,
                                            device_id={'dcp': dev}, device_id_type=pl.DeviceIdType.MESH)

    spans = ((0, AHEAD * GQ), (AHEAD * GQ, batch))

    def q_loads(n):
        span = slice(*spans[n])
        lat = [pltpu.make_async_copy(q_hbm.at[span, t, :, 0:LATENT], qall.at[k, c, span, :, t * LATENT:(t + 1) * LATENT], load_sem.at[n, t])
               for t in range(toks)]
        return lat, pltpu.make_async_copy(q_hbm.at[span, :, :, LATENT:LATENT + ROPE], rope_in.at[span], load_sem.at[n, toks])

    def q_ready(n):
        lat, rope = q_loads(n)
        span = slice(*spans[n])
        rope.wait()
        qall[k, c, span, :, toks * LATENT:] = jnp.concatenate([rope_in[span, t] for t in range(toks)], axis=-1)
        for cp in lat:
            cp.wait()

    def start(copies):
        for cp in copies:
            cp.start()

    def q_load(n):
        lat, rope = q_loads(n)
        start([rope] + lat)

    q_load(0)
    lengths = pltpu.make_async_copy(len_hbm, len_ref, len_sem)

    def kv_copy(b):
        slot = lax.rem(b, KV_SLOTS)
        return pltpu.make_async_copy(kv_hbm.at[b], kvb.at[slot], kv_sem.at[slot])

    def qreg(kk, cc, b0, n):
        return qall.at[kk, cc, pl.ds(b0, n)]

    def q_own(j):
        r = qreg(k, c, j * GQ, GQ)
        return [rcopy(r, r, qs.at[0, j], qr.at[0, j], right), rcopy(r, r, qs.at[1, j], qr.at[1, j], left),
                rcopy(r, r, qs.at[2, j], qr.at[2, j], partner)]

    def q_relay(j):
        lr, rr = qreg(k, cl, j * GQ, GQ), qreg(k, cr, j * GQ, GQ)
        lh, rh = qreg(k, cl, j * GQ, GQ // 2), qreg(k, cr, j * GQ + GQ // 2, GQ // 2)
        return [rcopy(lh, lh, qs.at[3, j], qr.at[3, j], right), rcopy(rh, rh, qs.at[4, j], qr.at[4, j], left),
                rcopy(lr, lr, qs.at[5, j], qr.at[5, j], partner), rcopy(rr, rr, qs.at[6, j], qr.at[6, j], partner)]

    def q_far(j):
        f0, f1 = qreg(k, cf, j * GQ, GQ // 2), qreg(k, cf, j * GQ + GQ // 2, GQ // 2)
        return [rcopy(f0, f0, qs.at[7, j], qr.at[7, j], partner), rcopy(f1, f1, qs.at[8, j], qr.at[8, j], partner)]

    def q_arrival(kind, j):
        full, h0, h1 = (j * GQ, GQ), (j * GQ, GQ // 2), (j * GQ + GQ // 2, GQ // 2)
        kk, cc, span = [(k, cl, full), (k, cr, full), (ok, c, full), (k, cf, h0), (k, cf, h1),
                        (ok, cl, full), (ok, cr, full), (ok, cf, h0), (ok, cf, h1)][kind]
        r = qreg(kk, cc, *span)
        return rcopy(r, r, qs.at[kind, j], qr.at[kind, j], partner)

    row_tok = (lax.broadcasted_iota(jnp.int32, (CORES * chips * rows, 1), 0) // heads) % toks
    key = lax.broadcasted_iota(jnp.int32, (1, npos), 1)
    pos = ((key // PAGE) * group + me) * PAGE + key % PAGE
    lanes = half * rows
    shift = lax.broadcasted_iota(jnp.int32, (chips * rows, lanes), 1) - lax.broadcasted_iota(jnp.int32, (chips * rows, lanes), 0) % rows
    lane_seq = lax.broadcasted_iota(jnp.int32, (chips, lanes), 1) // rows

    def scores(b):
        slot = lax.rem(b, KV_SLOTS)
        q = qall[:, :, b].reshape(CORES * chips, heads, toks * (LATENT + ROPE))
        lat = jnp.stack([q[:, :, t * LATENT:(t + 1) * LATENT] for t in range(toks)], axis=1).reshape(-1, LATENT)
        rope0 = toks * LATENT
        rope = jnp.stack([q[:, :, rope0 + t * ROPE:rope0 + (t + 1) * ROPE] for t in range(toks)], axis=1).reshape(-1, ROPE)
        q_rows = jnp.concatenate([lat, rope], axis=-1)
        return lax.dot_general(q_rows, kvb[slot], (((1,), (1,)), ((), ())), preferred_element_type=jnp.float32)

    def weights(b, s):
        s = jnp.where(pos <= len_ref[b] - toks + row_tok, s, -jnp.inf)
        m = jnp.max(s, axis=-1, keepdims=True)
        p = jnp.exp2((s - m) * SCALE2)
        return m, jnp.sum(p, axis=-1, keepdims=True), p.astype(jnp.bfloat16)

    def output(b, m, l, p):
        slot = lax.rem(b, KV_SLOTS)
        o = jnp.dot(p, kvb[slot, :, 0:LATENT], preferred_element_type=jnp.float32)
        o = (o * (1.0 / l)).astype(jnp.bfloat16)
        o_all[:, :, b] = o.reshape(CORES, chips, rows, LATENT)
        lse = m * SCALE2 + jnp.log2(l)
        place, in_half = b // half, b % half
        for kk in range(CORES):
            col = lse[kk * chips * rows:(kk + 1) * chips * rows]
            spread = jnp.where(shift == in_half * rows, col, 0.0).reshape(chips, rows, lanes)
            lse_all[kk, place] = jnp.where(lane_seq == in_half, jnp.sum(spread, axis=1), lse_all[kk, place])

    def attend(b0):
        bs_ = [b0 + u for u in range(UNROLL)]
        for b in bs_:
            kv_copy(b).wait()
        s = scores(bs_[0])
        for b in bs_:
            following = scores(b + 1) if b is not bs_[-1] else None
            output(b, *weights(b, s))
            s = following
        for b in bs_:
            @pl.when(b + KV_SLOTS < batch)
            def _():
                kv_copy(b + KV_SLOTS).start()

    def seqs(i, n=GO):
        return pl.ds(pl.multiple_of(i * n, n), n)

    def halves(i):
        return pl.ds(pl.multiple_of(2 * i, 2), 2)

    def columns(rows_):
        n = sum(r.shape[0] for r in rows_)
        return jnp.transpose(jnp.concatenate(rows_ + [jnp.zeros((8 - n, lanes), jnp.float32)] if n < 8 else rows_, axis=0))

    def merged(parts):
        top = functools.reduce(jnp.maximum, parts)
        total = top + jnp.log2(sum(jnp.exp2(x - top) for x in parts))
        return total, [jnp.exp2(x - total) for x in parts]

    def d_send(i):
        return [rcopy(o_all.at[ok, :, seqs(i)], prx.at[:, seqs(i)], ds.at[0, i], dr.at[0, i], partner),
                rcopy(lse_all.at[ok, halves(i)], plse.at[halves(i)], ds.at[1, i], dr.at[1, i], partner)]

    def d_merge(i):
        for cp in d_send(i):
            cp.wait_recv()
        w = []
        for h in range(2):
            total, (wa, wb) = merged([lse_all[k, 2 * i + h], plse[2 * i + h]])
            clse[2 * i + h] = total
            asnd[h, i] = clse[2 * i + h, pl.ds(cf, 1)]
            w.append(columns([wa, wb]))
        for j in range(GO):
            h, span = j // half, slice(j % half * rows, (j % half + 1) * rows)
            for cc in range(chips):
                x = o_all[k, cc, i * GO + j].astype(jnp.float32) * w[h][span, cc:cc + 1]
                y = prx[cc, i * GO + j].astype(jnp.float32) * w[h][span, chips + cc:chips + cc + 1]
                o_all[k, cc, i * GO + j] = (x + y).astype(jnp.bfloat16)

    def oreg(cc, i, part):
        if part is None:
            return o_all.at[k, cc, seqs(i)]
        return o_all.at[k, cc, pl.ds(i * GO + part * half, half)]

    def breg(side, i, part):
        return bbuf.at[side, pl.ds(i * GO + part * half, half)]

    def a_send(i):
        return [rcopy(oreg(cf, i, 0), abuf.at[0, pl.ds(i * half, half)], as_.at[0, i], ar.at[0, i], right),
                rcopy(oreg(cf, i, 1), abuf.at[1, pl.ds(i * half, half)], as_.at[1, i], ar.at[1, i], left),
                rcopy(asnd.at[0, i], alse.at[0, i], as_.at[2, i], ar.at[2, i], right),
                rcopy(asnd.at[1, i], alse.at[1, i], as_.at[3, i], ar.at[3, i], left)]

    def b_early(i):
        return [rcopy(oreg(cr, i, 1), breg(0, i, 1), bs.at[0, i], br.at[0, i], right),
                rcopy(oreg(cl, i, 0), breg(1, i, 0), bs.at[1, i], br.at[1, i], left)]

    def b_late(i):
        return [rcopy(bsnd.at[0, i], blse.at[0, i], bs.at[4, i], br.at[4, i], right),
                rcopy(bsnd.at[1, i], blse.at[1, i], bs.at[5, i], br.at[5, i], left),
                rcopy(oreg(cr, i, 0), breg(0, i, 0), bs.at[2, i], br.at[2, i], right),
                rcopy(oreg(cl, i, 1), breg(1, i, 1), bs.at[3, i], br.at[3, i], left)]

    def a_merge(i):
        for cp in a_send(i):
            cp.wait_recv()
        pl.when(i > 0)(lambda: start(b_late(i - 1)))
        w, fresh = [], []
        for side, cc in ((0, cr), (1, cl)):
            total, both = merged([clse[2 * i + side, pl.ds(cc, 1)], alse[side, i]])
            fresh.append(total)
            w += both
        bsnd[0, i] = jnp.concatenate([fresh[0], clse[2 * i + 1, pl.ds(cr, 1)]], axis=0)
        bsnd[1, i] = jnp.concatenate([clse[2 * i, pl.ds(cl, 1)], fresh[1]], axis=0)
        w = columns(w)
        for side, cc in ((0, cr), (1, cl)):
            for j in range(half):
                b, span = i * GO + side * half + j, slice(j * rows, (j + 1) * rows)
                x = o_all[k, cc, b].astype(jnp.float32) * w[span, 2 * side:2 * side + 1]
                y = abuf[side, i * half + j].astype(jnp.float32) * w[span, 2 * side + 1:2 * side + 2]
                o_all[k, cc, b] = (x + y).astype(jnp.bfloat16)

    def final_merge(i):
        late = b_late(i)
        for cp in b_early(i) + late[:2]:
            cp.wait_recv()
        own = jnp.concatenate([clse[2 * i + h, pl.ds(c, 1)] for h in range(2)], axis=0)
        w = columns(merged([own, blse[0, i], blse[1, i]])[1])
        for h in range(2):
            late[2 + h].wait_recv()
            for j in range(half):
                b, span = i * GO + h * half + j, slice(j * rows, (j + 1) * rows)
                x = o_all[k, c, b].astype(jnp.float32) * w[span, h:h + 1]
                x += bbuf[0, b].astype(jnp.float32) * w[span, 2 + h:3 + h]
                x += bbuf[1, b].astype(jnp.float32) * w[span, 4 + h:5 + h]
                out_ref[b] = x.astype(jnp.bfloat16)
        sent(late)

    def sent(copies):
        for cp in copies:
            cp.wait_send()

    def ring_start(lo, hi):
        lax.fori_loop(lo, hi, lambda i, carry: (start(a_send(i) + b_early(i)), carry)[1], 0)

    q_ready(0)
    pl.semaphore_wait(barrier, 3)
    for j in range(AHEAD):
        start(q_own(j))
    q_load(1)
    lengths.start()
    for b in range(KV_SLOTS):
        kv_copy(b).start()
    q_ready(1)
    lengths.wait()

    def step(j, carry):
        @pl.when(j < n_q)
        def _():
            q_arrival(0, j).wait_recv()
            q_arrival(1, j).wait_recv()
            for cp in q_relay(j):
                cp.start()

        @pl.when(j + AHEAD < n_q)
        def _():
            for cp in q_own(j + AHEAD):
                cp.start()

        @pl.when((j >= 1) & (j <= n_q))
        def _():
            q_arrival(3, j - 1).wait_recv()
            q_arrival(4, j - 1).wait_recv()
            for cp in q_far(j - 1):
                cp.start()

        for at, op in enumerate((lambda: start(a_send(0)), lambda: start(b_early(0)), lambda: ring_start(1, 2), lambda: ring_start(2, n_o // 2),
                                 lambda: ring_start(n_o // 2, n_o - 2), lambda: ring_start(n_o - 2, n_o - 1))):
            pl.when(j == n_q - 4 + at)(op)

        @pl.when((j >= 4) & (j % 2 == 0))
        def _():
            start(d_send(j // 2 - 2))

        @pl.when(j >= 2)
        def _():
            s = j - 2
            for kind in (2, 5, 6, 7, 8):
                q_arrival(kind, s).wait_recv()
            lax.fori_loop(0, GQ // UNROLL, lambda n, cc: (attend(s * GQ + n * UNROLL), cc)[1], 0)

            @pl.when((s % 2 == 0) & (s > 0))
            def _():
                d_merge(s // 2 - 1)

        return carry

    def each(lo, hi, op):
        lax.fori_loop(lo, hi, lambda i, carry: (op(i), carry)[1], 0)

    each(0, n_q + 2, lambda j: step(j, 0))
    each(0, n_q // 2, lambda j: sent(q_own(j) + q_relay(j) + q_far(j)))
    start(d_send(n_o - 1))
    d_merge(n_o - 1)
    each(n_q // 2, n_q, lambda j: sent(q_own(j) + q_relay(j) + q_far(j)))
    ring_start(n_o - 1, n_o)
    each(0, n_o, a_merge)
    each(0, n_o, lambda i: sent(d_send(i)))
    start(b_late(n_o - 1))
    each(0, n_o, lambda i: sent(a_send(i) + b_early(i)))
    each(0, n_o, final_merge)


def solution(mesh):
    group = mesh.shape['dcp']
    chips = group // CORES

    def local_step(q_blk, kv_blk, len_blk):
        batch, toks, heads, width = q_blk.shape
        npos = kv_blk.shape[1] * kv_blk.shape[2] * kv_blk.shape[3]
        rows, lanes = toks * heads, GO // 2 * toks * heads
        n_q, n_o = batch // GQ, batch // GO
        bf16, f32, dma = jnp.bfloat16, jnp.float32, pltpu.SemaphoreType.DMA
        any_space = pl.BlockSpec(memory_space=pl.ANY)
        out = pl.pallas_call(
            functools.partial(_kernel, (batch, toks, heads, npos, group)),
            out_shape=pltpu.VMEM((batch, rows, LATENT), bf16),
            in_specs=[any_space, any_space, any_space],
            out_specs=pl.BlockSpec(memory_space=pltpu.VMEM),
            scratch_shapes=[
                pltpu.SMEM((batch,), jnp.int32),
                pltpu.VMEM((CORES, chips, batch, heads, toks * width), bf16),
                pltpu.VMEM((batch, toks, heads, ROPE), bf16),
                pltpu.VMEM((KV_SLOTS, npos, width), bf16),
                pltpu.VMEM((CORES, chips, batch, rows, LATENT), bf16),
                pltpu.VMEM((chips, batch, rows, LATENT), bf16),
                pltpu.VMEM((2, batch // 2, rows, LATENT), bf16),
                pltpu.VMEM((2, batch, rows, LATENT), bf16),
                pltpu.VMEM((CORES, 2 * n_o, chips, lanes), f32),
                pltpu.VMEM((2 * n_o, chips, lanes), f32),
                pltpu.VMEM((2 * n_o, chips, lanes), f32),
                pltpu.VMEM((2, n_o, 1, lanes), f32),
                pltpu.VMEM((2, n_o, 1, lanes), f32),
                pltpu.VMEM((2, n_o, 2, lanes), f32),
                pltpu.VMEM((2, n_o, 2, lanes), f32),
                dma((2, toks + 1)), dma, dma((KV_SLOTS,)),
                dma((9, n_q)), dma((9, n_q)),
                dma((2, n_o)), dma((2, n_o)),
                dma((4, n_o)), dma((4, n_o)),
                dma((6, n_o)), dma((6, n_o)),
            ],
            compiler_params=pltpu.CompilerParams(collective_id=0, has_side_effects=True, vmem_limit_bytes=63_000_000),
            name='mla_ring',
        )(q_blk, kv_blk.reshape(batch, npos, width), len_blk)
        return out.reshape(batch, toks, heads, LATENT)

    return jax.shard_map(local_step, mesh=mesh, in_specs=(P('dp', None, 'dcp', None), P('dp', None, 'dcp', None, None), P('dp')),
                         out_specs=P('dp', None, 'dcp', None), check_vma=False)
```

```python
import functools
import math

import jax
import jax.numpy as jnp
from jax import lax
from jax.experimental import pallas as pl
from jax.experimental.pallas import tpu as pltpu
from jax.sharding import PartitionSpec as P

LATENT = 512
ROPE = 64
NOPE = 128
PAGE = 64
CORES = 2
SCALE2 = (NOPE + ROPE) ** -0.5 * math.log2(math.e)

GQ = 4
GO = 8
KV_SLOTS = 4
OUT_COPIES = 4
UNROLL = 2
AHEAD = 3


def _kernel(sizes, q_hbm, kv_hbm, len_hbm, out_ref,
            len_ref, qall, rope_in, kvb, o_all, prx, abuf, bbuf,
            lse_all, plse, clse, asnd, alse, bsnd, blse,
            load_sem, len_sem, kv_sem, qs, qr, ds, dr, as_, ar, bs, br):
    batch, toks, heads, npos, group = sizes
    chips = group // CORES
    rows = toks * heads
    half = GO // 2
    n_q, n_o = batch // GQ, batch // GO
    me = lax.axis_index('dcp')
    c, k = me // CORES, me % CORES
    ok = 1 - k
    cr, cl, cf = (c + 1) % chips, (c + chips - 1) % chips, (c + 2) % chips
    right, left, partner = cr * CORES + k, cl * CORES + k, c * CORES + ok

    barrier = pltpu.get_barrier_semaphore()
    for other in (right, left, partner):
        pl.semaphore_signal(barrier, inc=1, device_id={'dcp': other}, device_id_type=pl.DeviceIdType.MESH)

    def rcopy(src, dst, send, recv, dev):
        return pltpu.make_async_remote_copy(src_ref=src, dst_ref=dst, send_sem=send, recv_sem=recv,
                                            device_id={'dcp': dev}, device_id_type=pl.DeviceIdType.MESH)

    spans = ((0, AHEAD * GQ), (AHEAD * GQ, batch))

    def q_loads(n):
        span = slice(*spans[n])
        lat = [pltpu.make_async_copy(q_hbm.at[span, t, :, 0:LATENT], qall.at[k, c, span, :, t * LATENT:(t + 1) * LATENT], load_sem.at[n, t])
               for t in range(toks)]
        return lat, pltpu.make_async_copy(q_hbm.at[span, :, :, LATENT:LATENT + ROPE], rope_in.at[span], load_sem.at[n, toks])

    def q_ready(n):
        lat, rope = q_loads(n)
        span = slice(*spans[n])
        rope.wait()
        qall[k, c, span, :, toks * LATENT:] = jnp.concatenate([rope_in[span, t] for t in range(toks)], axis=-1)
        for cp in lat:
            cp.wait()

    def start(copies):
        for cp in copies:
            cp.start()

    def q_load(n):
        lat, rope = q_loads(n)
        start([rope] + lat)

    q_load(0)
    lengths = pltpu.make_async_copy(len_hbm, len_ref, len_sem)

    def kv_copy(b):
        slot = lax.rem(b, KV_SLOTS)
        return pltpu.make_async_copy(kv_hbm.at[b], kvb.at[slot], kv_sem.at[slot])

    def qreg(kk, cc, b0, n):
        return qall.at[kk, cc, pl.ds(b0, n)]

    def q_own(j):
        r = qreg(k, c, j * GQ, GQ)
        return [rcopy(r, r, qs.at[0, j], qr.at[0, j], right), rcopy(r, r, qs.at[1, j], qr.at[1, j], left),
                rcopy(r, r, qs.at[2, j], qr.at[2, j], partner)]

    def q_relay(j):
        lr, rr = qreg(k, cl, j * GQ, GQ), qreg(k, cr, j * GQ, GQ)
        lh, rh = qreg(k, cl, j * GQ, GQ // 2), qreg(k, cr, j * GQ + GQ // 2, GQ // 2)
        return [rcopy(lh, lh, qs.at[3, j], qr.at[3, j], right), rcopy(rh, rh, qs.at[4, j], qr.at[4, j], left),
                rcopy(lr, lr, qs.at[5, j], qr.at[5, j], partner), rcopy(rr, rr, qs.at[6, j], qr.at[6, j], partner)]

    def q_far(j):
        f0, f1 = qreg(k, cf, j * GQ, GQ // 2), qreg(k, cf, j * GQ + GQ // 2, GQ // 2)
        return [rcopy(f0, f0, qs.at[7, j], qr.at[7, j], partner), rcopy(f1, f1, qs.at[8, j], qr.at[8, j], partner)]

    def q_arrival(kind, j):
        full, h0, h1 = (j * GQ, GQ), (j * GQ, GQ // 2), (j * GQ + GQ // 2, GQ // 2)
        kk, cc, span = [(k, cl, full), (k, cr, full), (ok, c, full), (k, cf, h0), (k, cf, h1),
                        (ok, cl, full), (ok, cr, full), (ok, cf, h0), (ok, cf, h1)][kind]
        r = qreg(kk, cc, *span)
        return rcopy(r, r, qs.at[kind, j], qr.at[kind, j], partner)

    row_tok = (lax.broadcasted_iota(jnp.int32, (CORES * chips * rows, 1), 0) // heads) % toks
    key = lax.broadcasted_iota(jnp.int32, (1, npos), 1)
    pos = ((key // PAGE) * group + me) * PAGE + key % PAGE
    lanes = half * rows
    shift = lax.broadcasted_iota(jnp.int32, (chips * rows, lanes), 1) - lax.broadcasted_iota(jnp.int32, (chips * rows, lanes), 0) % rows
    lane_seq = lax.broadcasted_iota(jnp.int32, (chips, lanes), 1) // rows

    def scores(b):
        slot = lax.rem(b, KV_SLOTS)
        q = qall[:, :, b].reshape(CORES * chips, heads, toks * (LATENT + ROPE))
        lat = jnp.stack([q[:, :, t * LATENT:(t + 1) * LATENT] for t in range(toks)], axis=1).reshape(-1, LATENT)
        rope0 = toks * LATENT
        rope = jnp.stack([q[:, :, rope0 + t * ROPE:rope0 + (t + 1) * ROPE] for t in range(toks)], axis=1).reshape(-1, ROPE)
        q_rows = jnp.concatenate([lat, rope], axis=-1)
        return lax.dot_general(q_rows, kvb[slot], (((1,), (1,)), ((), ())), preferred_element_type=jnp.float32)

    def weights(b, s):
        s = jnp.where(pos <= len_ref[b] - toks + row_tok, s, -jnp.inf)
        m = jnp.max(s, axis=-1, keepdims=True)
        p = jnp.exp2((s - m) * SCALE2)
        return m, jnp.sum(p, axis=-1, keepdims=True), p.astype(jnp.bfloat16)

    def output(b, m, l, p):
        slot = lax.rem(b, KV_SLOTS)
        o = jnp.dot(p, kvb[slot, :, 0:LATENT], preferred_element_type=jnp.float32)
        o = (o * (1.0 / l)).astype(jnp.bfloat16)
        o_all[:, :, b] = o.reshape(CORES, chips, rows, LATENT)
        lse = m * SCALE2 + jnp.log2(l)
        place, in_half = b // half, b % half
        for kk in range(CORES):
            col = lse[kk * chips * rows:(kk + 1) * chips * rows]
            spread = jnp.where(shift == in_half * rows, col, 0.0).reshape(chips, rows, lanes)
            lse_all[kk, place] = jnp.where(lane_seq == in_half, jnp.sum(spread, axis=1), lse_all[kk, place])

    def attend(b0):
        bs_ = [b0 + u for u in range(UNROLL)]
        for b in bs_:
            kv_copy(b).wait()
        s = scores(bs_[0])
        for b in bs_:
            following = scores(b + 1) if b is not bs_[-1] else None
            output(b, *weights(b, s))
            s = following
        for b in bs_:
            @pl.when(b + KV_SLOTS < batch)
            def _():
                kv_copy(b + KV_SLOTS).start()

    def seqs(i, n=GO):
        return pl.ds(pl.multiple_of(i * n, n), n)

    def halves(i):
        return pl.ds(pl.multiple_of(2 * i, 2), 2)

    def columns(rows_):
        n = sum(r.shape[0] for r in rows_)
        return jnp.transpose(jnp.concatenate(rows_ + [jnp.zeros((8 - n, lanes), jnp.float32)] if n < 8 else rows_, axis=0))

    def merged(parts):
        top = functools.reduce(jnp.maximum, parts)
        total = top + jnp.log2(sum(jnp.exp2(x - top) for x in parts))
        return total, [jnp.exp2(x - total) for x in parts]

    def d_send(i):
        return [rcopy(o_all.at[ok, :, seqs(i)], prx.at[:, seqs(i)], ds.at[0, i], dr.at[0, i], partner),
                rcopy(lse_all.at[ok, halves(i)], plse.at[halves(i)], ds.at[1, i], dr.at[1, i], partner)]

    def d_merge(i):
        for cp in d_send(i):
            cp.wait_recv()
        w = []
        for h in range(2):
            total, (wa, wb) = merged([lse_all[k, 2 * i + h], plse[2 * i + h]])
            clse[2 * i + h] = total
            asnd[h, i] = clse[2 * i + h, pl.ds(cf, 1)]
            w.append(columns([wa, wb]))
        for j in range(GO):
            h, span = j // half, slice(j % half * rows, (j % half + 1) * rows)
            for cc in range(chips):
                x = o_all[k, cc, i * GO + j].astype(jnp.float32) * w[h][span, cc:cc + 1]
                y = prx[cc, i * GO + j].astype(jnp.float32) * w[h][span, chips + cc:chips + cc + 1]
                o_all[k, cc, i * GO + j] = (x + y).astype(jnp.bfloat16)

    def oreg(cc, i, part):
        if part is None:
            return o_all.at[k, cc, seqs(i)]
        return o_all.at[k, cc, pl.ds(i * GO + part * half, half)]

    def breg(side, i, part):
        return bbuf.at[side, pl.ds(i * GO + part * half, half)]

    def a_send(i):
        return [rcopy(oreg(cf, i, 0), abuf.at[0, pl.ds(i * half, half)], as_.at[0, i], ar.at[0, i], right),
                rcopy(oreg(cf, i, 1), abuf.at[1, pl.ds(i * half, half)], as_.at[1, i], ar.at[1, i], left),
                rcopy(asnd.at[0, i], alse.at[0, i], as_.at[2, i], ar.at[2, i], right),
                rcopy(asnd.at[1, i], alse.at[1, i], as_.at[3, i], ar.at[3, i], left)]

    def b_early(i):
        return [rcopy(oreg(cr, i, 1), breg(0, i, 1), bs.at[0, i], br.at[0, i], right),
                rcopy(oreg(cl, i, 0), breg(1, i, 0), bs.at[1, i], br.at[1, i], left)]

    def b_late(i):
        return [rcopy(bsnd.at[0, i], blse.at[0, i], bs.at[4, i], br.at[4, i], right),
                rcopy(bsnd.at[1, i], blse.at[1, i], bs.at[5, i], br.at[5, i], left),
                rcopy(oreg(cr, i, 0), breg(0, i, 0), bs.at[2, i], br.at[2, i], right),
                rcopy(oreg(cl, i, 1), breg(1, i, 1), bs.at[3, i], br.at[3, i], left)]

    def a_merge(i):
        for cp in a_send(i):
            cp.wait_recv()
        pl.when(i > 0)(lambda: start(b_late(i - 1)))
        w, fresh = [], []
        for side, cc in ((0, cr), (1, cl)):
            total, both = merged([clse[2 * i + side, pl.ds(cc, 1)], alse[side, i]])
            fresh.append(total)
            w += both
        bsnd[0, i] = jnp.concatenate([fresh[0], clse[2 * i + 1, pl.ds(cr, 1)]], axis=0)
        bsnd[1, i] = jnp.concatenate([clse[2 * i, pl.ds(cl, 1)], fresh[1]], axis=0)
        w = columns(w)
        for side, cc in ((0, cr), (1, cl)):
            for j in range(half):
                b, span = i * GO + side * half + j, slice(j * rows, (j + 1) * rows)
                x = o_all[k, cc, b].astype(jnp.float32) * w[span, 2 * side:2 * side + 1]
                y = abuf[side, i * half + j].astype(jnp.float32) * w[span, 2 * side + 1:2 * side + 2]
                o_all[k, cc, b] = (x + y).astype(jnp.bfloat16)

    def final_merge(i):
        late = b_late(i)
        for cp in b_early(i) + late[:2]:
            cp.wait_recv()
        own = jnp.concatenate([clse[2 * i + h, pl.ds(c, 1)] for h in range(2)], axis=0)
        w = columns(merged([own, blse[0, i], blse[1, i]])[1])
        for h in range(2):
            late[2 + h].wait_recv()
            for j in range(half):
                b, span = i * GO + h * half + j, slice(j * rows, (j + 1) * rows)
                x = o_all[k, c, b].astype(jnp.float32) * w[span, h:h + 1]
                x += bbuf[0, b].astype(jnp.float32) * w[span, 2 + h:3 + h]
                x += bbuf[1, b].astype(jnp.float32) * w[span, 4 + h:5 + h]
                out_ref[b] = x.astype(jnp.bfloat16)
        sent(late)

    def sent(copies):
        for cp in copies:
            cp.wait_send()

    def ring_start(lo, hi):
        lax.fori_loop(lo, hi, lambda i, carry: (start(a_send(i) + b_early(i)), carry)[1], 0)

    q_ready(0)
    pl.semaphore_wait(barrier, 3)
    for j in range(AHEAD):
        start(q_own(j))
    q_load(1)
    lengths.start()
    for b in range(KV_SLOTS):
        kv_copy(b).start()
    q_ready(1)
    lengths.wait()

    def step(j, carry):
        @pl.when(j < n_q)
        def _():
            q_arrival(0, j).wait_recv()
            q_arrival(1, j).wait_recv()
            for cp in q_relay(j):
                cp.start()

        @pl.when(j + AHEAD < n_q)
        def _():
            for cp in q_own(j + AHEAD):
                cp.start()

        @pl.when((j >= 1) & (j <= n_q))
        def _():
            q_arrival(3, j - 1).wait_recv()
            q_arrival(4, j - 1).wait_recv()
            for cp in q_far(j - 1):
                cp.start()

        for at, op in enumerate((lambda: start(a_send(0)), lambda: start(b_early(0)), lambda: ring_start(1, 2), lambda: ring_start(2, n_o // 2),
                                 lambda: ring_start(n_o // 2, n_o - 2), lambda: ring_start(n_o - 2, n_o - 1))):
            pl.when(j == n_q - 4 + at)(op)

        @pl.when((j >= 4) & (j % 2 == 0))
        def _():
            start(d_send(j // 2 - 2))

        @pl.when(j >= 2)
        def _():
            s = j - 2
            for kind in (2, 5, 6, 7, 8):
                q_arrival(kind, s).wait_recv()
            lax.fori_loop(0, GQ // UNROLL, lambda n, cc: (attend(s * GQ + n * UNROLL), cc)[1], 0)

            @pl.when((s % 2 == 0) & (s > 0))
            def _():
                d_merge(s // 2 - 1)

        return carry

    def each(lo, hi, op):
        lax.fori_loop(lo, hi, lambda i, carry: (op(i), carry)[1], 0)

    each(0, n_q + 2, lambda j: step(j, 0))
    each(0, n_q // 2, lambda j: sent(q_own(j) + q_relay(j) + q_far(j)))
    start(d_send(n_o - 1))
    d_merge(n_o - 1)
    each(n_q // 2, n_q, lambda j: sent(q_own(j) + q_relay(j) + q_far(j)))
    ring_start(n_o - 1, n_o)
    each(0, n_o, a_merge)
    each(0, n_o, lambda i: sent(d_send(i)))
    start(b_late(n_o - 1))
    each(0, n_o, lambda i: sent(a_send(i) + b_early(i)))
    each(0, n_o, final_merge)


def _write_out(src, dst, sem):
    n = src.shape[0] // OUT_COPIES
    copies = [pltpu.make_async_copy(src.at[pl.ds(i * n, n)], dst.at[pl.ds(i * n, n)], sem.at[i]) for i in range(OUT_COPIES)]
    for cp in copies:
        cp.start()
    for cp in copies:
        cp.wait()


def solution(mesh):
    group = mesh.shape['dcp']
    chips = group // CORES

    def local_step(q_blk, kv_blk, len_blk):
        batch, toks, heads, width = q_blk.shape
        npos = kv_blk.shape[1] * kv_blk.shape[2] * kv_blk.shape[3]
        rows, lanes = toks * heads, GO // 2 * toks * heads
        n_q, n_o = batch // GQ, batch // GO
        bf16, f32, dma = jnp.bfloat16, jnp.float32, pltpu.SemaphoreType.DMA
        any_space = pl.BlockSpec(memory_space=pl.ANY)
        out = pl.pallas_call(
            functools.partial(_kernel, (batch, toks, heads, npos, group)),
            out_shape=pltpu.VMEM((batch, rows, LATENT), bf16),
            in_specs=[any_space, any_space, any_space],
            out_specs=pl.BlockSpec(memory_space=pltpu.VMEM),
            scratch_shapes=[
                pltpu.SMEM((batch,), jnp.int32),
                pltpu.VMEM((CORES, chips, batch, heads, toks * width), bf16),
                pltpu.VMEM((batch, toks, heads, ROPE), bf16),
                pltpu.VMEM((KV_SLOTS, npos, width), bf16),
                pltpu.VMEM((CORES, chips, batch, rows, LATENT), bf16),
                pltpu.VMEM((chips, batch, rows, LATENT), bf16),
                pltpu.VMEM((2, batch // 2, rows, LATENT), bf16),
                pltpu.VMEM((2, batch, rows, LATENT), bf16),
                pltpu.VMEM((CORES, 2 * n_o, chips, lanes), f32),
                pltpu.VMEM((2 * n_o, chips, lanes), f32),
                pltpu.VMEM((2 * n_o, chips, lanes), f32),
                pltpu.VMEM((2, n_o, 1, lanes), f32),
                pltpu.VMEM((2, n_o, 1, lanes), f32),
                pltpu.VMEM((2, n_o, 2, lanes), f32),
                pltpu.VMEM((2, n_o, 2, lanes), f32),
                dma((2, toks + 1)), dma, dma((KV_SLOTS,)),
                dma((9, n_q)), dma((9, n_q)),
                dma((2, n_o)), dma((2, n_o)),
                dma((4, n_o)), dma((4, n_o)),
                dma((6, n_o)), dma((6, n_o)),
            ],
            compiler_params=pltpu.CompilerParams(collective_id=0, has_side_effects=True, vmem_limit_bytes=63_000_000),
            name='mla_ring',
        )(q_blk, kv_blk.reshape(batch, npos, width), len_blk)
        return pl.pallas_call(
            _write_out,
            out_shape=jax.ShapeDtypeStruct((batch, rows, LATENT), bf16),
            in_specs=[pl.BlockSpec(memory_space=pltpu.VMEM)],
            out_specs=any_space,
            scratch_shapes=[dma((OUT_COPIES,))],
            name='write_out',
        )(pltpu.with_memory_space_constraint(out, pltpu.VMEM)).reshape(batch, toks, heads, LATENT)

    return jax.shard_map(local_step, mesh=mesh, in_specs=(P('dp', None, 'dcp', None), P('dp', None, 'dcp', None, None), P('dp')),
                         out_specs=P('dp', None, 'dcp', None), check_vma=False)
```

```python
import functools
import math

import jax
import jax.numpy as jnp
from jax import lax
from jax.experimental import pallas as pl
from jax.experimental.pallas import tpu as pltpu
from jax.sharding import PartitionSpec as P

LATENT = 512
ROPE = 64
NOPE = 128
PAGE = 64
CORES = 2
SCALE2 = (NOPE + ROPE) ** -0.5 * math.log2(math.e)

GQ = 4
GO = 8
KV_SLOTS = 4
UNROLL = 2
AHEAD = 3


def _kernel(sizes, q_hbm, kv_hbm, len_hbm, out_ref,
            len_ref, qall, rope_in, kvb, o_all, prx, abuf, bbuf,
            lse_all, plse, clse, asnd, alse, bsnd, blse,
            load_sem, len_sem, kv_sem, qs, qr, ds, dr, as_, ar, bs, br):
    batch, toks, heads, npos, group = sizes
    chips = group // CORES
    rows = toks * heads
    half = GO // 2
    n_q, n_o = batch // GQ, batch // GO
    lse_group = n_o // 2
    me = lax.axis_index('dcp')
    c, k = me // CORES, me % CORES
    ok = 1 - k
    cr, cl, cf = (c + 1) % chips, (c + chips - 1) % chips, (c + 2) % chips
    right, left, partner = cr * CORES + k, cl * CORES + k, c * CORES + ok

    barrier = pltpu.get_barrier_semaphore()
    for other in (right, left, partner):
        pl.semaphore_signal(barrier, inc=1, device_id={'dcp': other}, device_id_type=pl.DeviceIdType.MESH)

    def rcopy(src, dst, send, recv, dev):
        return pltpu.make_async_remote_copy(src_ref=src, dst_ref=dst, send_sem=send, recv_sem=recv,
                                            device_id={'dcp': dev}, device_id_type=pl.DeviceIdType.MESH)

    spans = ((0, AHEAD * GQ), (AHEAD * GQ, batch))

    def q_loads(n):
        span = slice(*spans[n])
        lat = [pltpu.make_async_copy(q_hbm.at[span, t, :, 0:LATENT], qall.at[k, c, span, :, t * LATENT:(t + 1) * LATENT], load_sem.at[n, t])
               for t in range(toks)]
        return lat, pltpu.make_async_copy(q_hbm.at[span, :, :, LATENT:LATENT + ROPE], rope_in.at[span], load_sem.at[n, toks])

    def q_ready(n):
        lat, rope = q_loads(n)
        span = slice(*spans[n])
        rope.wait()
        qall[k, c, span, :, toks * LATENT:] = jnp.concatenate([rope_in[span, t] for t in range(toks)], axis=-1)
        for cp in lat:
            cp.wait()

    def start(copies):
        for cp in copies:
            cp.start()

    def q_load(n):
        lat, rope = q_loads(n)
        start([rope] + lat)

    q_load(0)
    lengths = pltpu.make_async_copy(len_hbm, len_ref, len_sem)

    def kv_copy(b):
        slot = lax.rem(b, KV_SLOTS)
        return pltpu.make_async_copy(kv_hbm.at[b], kvb.at[slot], kv_sem.at[slot])

    def qreg(kk, cc, b0, n):
        return qall.at[kk, cc, pl.ds(b0, n)]

    def q_own(j):
        r = qreg(k, c, j * GQ, GQ)
        return [rcopy(r, r, qs.at[0, j], qr.at[0, j], right), rcopy(r, r, qs.at[1, j], qr.at[1, j], left),
                rcopy(r, r, qs.at[2, j], qr.at[2, j], partner)]

    def q_relay(j):
        lr, rr = qreg(k, cl, j * GQ, GQ), qreg(k, cr, j * GQ, GQ)
        lh, rh = qreg(k, cl, j * GQ, GQ // 2), qreg(k, cr, j * GQ + GQ // 2, GQ // 2)
        return [rcopy(lh, lh, qs.at[3, j], qr.at[3, j], right), rcopy(rh, rh, qs.at[4, j], qr.at[4, j], left),
                rcopy(lr, lr, qs.at[5, j], qr.at[5, j], partner), rcopy(rr, rr, qs.at[6, j], qr.at[6, j], partner)]

    def q_far(j):
        f0, f1 = qreg(k, cf, j * GQ, GQ // 2), qreg(k, cf, j * GQ + GQ // 2, GQ // 2)
        return [rcopy(f0, f0, qs.at[7, j], qr.at[7, j], partner), rcopy(f1, f1, qs.at[8, j], qr.at[8, j], partner)]

    def q_arrival(kind, j):
        full, h0, h1 = (j * GQ, GQ), (j * GQ, GQ // 2), (j * GQ + GQ // 2, GQ // 2)
        kk, cc, span = [(k, cl, full), (k, cr, full), (ok, c, full), (k, cf, h0), (k, cf, h1),
                        (ok, cl, full), (ok, cr, full), (ok, cf, h0), (ok, cf, h1)][kind]
        r = qreg(kk, cc, *span)
        return rcopy(r, r, qs.at[kind, j], qr.at[kind, j], partner)

    row_tok = (lax.broadcasted_iota(jnp.int32, (CORES * chips * rows, 1), 0) // heads) % toks
    key = lax.broadcasted_iota(jnp.int32, (1, npos), 1)
    pos = ((key // PAGE) * group + me) * PAGE + key % PAGE
    lanes = half * rows
    shift = lax.broadcasted_iota(jnp.int32, (chips * rows, lanes), 1) - lax.broadcasted_iota(jnp.int32, (chips * rows, lanes), 0) % rows
    lane_seq = lax.broadcasted_iota(jnp.int32, (chips, lanes), 1) // rows

    def scores(b):
        slot = lax.rem(b, KV_SLOTS)
        q = qall[:, :, b].reshape(CORES * chips, heads, toks * (LATENT + ROPE))
        lat = jnp.stack([q[:, :, t * LATENT:(t + 1) * LATENT] for t in range(toks)], axis=1).reshape(-1, LATENT)
        rope0 = toks * LATENT
        rope = jnp.stack([q[:, :, rope0 + t * ROPE:rope0 + (t + 1) * ROPE] for t in range(toks)], axis=1).reshape(-1, ROPE)
        q_rows = jnp.concatenate([lat, rope], axis=-1)
        return lax.dot_general(q_rows, kvb[slot], (((1,), (1,)), ((), ())), preferred_element_type=jnp.float32)

    def weights(b, s):
        s = jnp.where(pos <= len_ref[b] - toks + row_tok, s, -jnp.inf)
        m = jnp.max(s, axis=-1, keepdims=True)
        p = jnp.exp2((s - m) * SCALE2)
        return m, jnp.sum(p, axis=-1, keepdims=True), p.astype(jnp.bfloat16)

    def output(b, m, l, p):
        slot = lax.rem(b, KV_SLOTS)
        o = jnp.dot(p, kvb[slot, :, 0:LATENT], preferred_element_type=jnp.float32)
        o = (o * (1.0 / l)).astype(jnp.bfloat16)
        o_all[:, :, b] = o.reshape(CORES, chips, rows, LATENT)
        lse = m * SCALE2 + jnp.log2(l)
        place, in_half = b // half, b % half
        for kk in range(CORES):
            col = lse[kk * chips * rows:(kk + 1) * chips * rows]
            spread = jnp.where(shift == in_half * rows, col, 0.0).reshape(chips, rows, lanes)
            lse_all[kk, place] = jnp.where(lane_seq == in_half, jnp.sum(spread, axis=1), lse_all[kk, place])

    def attend(b0):
        bs_ = [b0 + u for u in range(UNROLL)]
        for b in bs_:
            kv_copy(b).wait()
        s = scores(bs_[0])
        for b in bs_:
            following = scores(b + 1) if b is not bs_[-1] else None
            output(b, *weights(b, s))
            s = following
        for b in bs_:
            @pl.when(b + KV_SLOTS < batch)
            def _():
                kv_copy(b + KV_SLOTS).start()

    def seqs(i, n=GO):
        return pl.ds(pl.multiple_of(i * n, n), n)

    def halves(i):
        return pl.ds(pl.multiple_of(2 * i, 2), 2)

    def columns(rows_):
        n = sum(r.shape[0] for r in rows_)
        return jnp.transpose(jnp.concatenate(rows_ + [jnp.zeros((8 - n, lanes), jnp.float32)] if n < 8 else rows_, axis=0))

    def merged(parts):
        top = functools.reduce(jnp.maximum, parts)
        total = top + jnp.log2(sum(jnp.exp2(x - top) for x in parts))
        return total, [jnp.exp2(x - total) for x in parts]

    def d_send(i):
        return [rcopy(o_all.at[ok, :, seqs(i)], prx.at[:, seqs(i)], ds.at[0, i], dr.at[0, i], partner),
                rcopy(lse_all.at[ok, halves(i)], plse.at[halves(i)], ds.at[1, i], dr.at[1, i], partner)]

    def d_merge(i):
        for cp in d_send(i):
            cp.wait_recv()
        w = []
        for h in range(2):
            total, (wa, wb) = merged([lse_all[k, 2 * i + h], plse[2 * i + h]])
            clse[2 * i + h] = total
            asnd[h, i] = clse[2 * i + h, pl.ds(cf, 1)]
            w.append(columns([wa, wb]))
        for j in range(GO):
            h, span = j // half, slice(j % half * rows, (j % half + 1) * rows)
            for cc in range(chips):
                x = o_all[k, cc, i * GO + j].astype(jnp.float32) * w[h][span, cc:cc + 1]
                y = prx[cc, i * GO + j].astype(jnp.float32) * w[h][span, chips + cc:chips + cc + 1]
                o_all[k, cc, i * GO + j] = (x + y).astype(jnp.bfloat16)

    def oreg(cc, i, part):
        if part is None:
            return o_all.at[k, cc, seqs(i)]
        return o_all.at[k, cc, pl.ds(i * GO + part * half, half)]

    def breg(side, i, part):
        return bbuf.at[side, pl.ds(i * GO + part * half, half)]

    def a_send(i):
        return [rcopy(oreg(cf, i, 0), abuf.at[0, pl.ds(i * half, half)], as_.at[0, i], ar.at[0, i], right),
                rcopy(oreg(cf, i, 1), abuf.at[1, pl.ds(i * half, half)], as_.at[1, i], ar.at[1, i], left)]

    def group_of(g):
        return pl.ds(g * lse_group, lse_group)

    def a_lse(g):
        return [rcopy(asnd.at[0, group_of(g)], alse.at[0, group_of(g)], as_.at[2, g], ar.at[2, g], right),
                rcopy(asnd.at[1, group_of(g)], alse.at[1, group_of(g)], as_.at[3, g], ar.at[3, g], left)]

    def b_lse(g):
        return [rcopy(bsnd.at[0, group_of(g)], blse.at[0, group_of(g)], bs.at[4, g], br.at[4, g], right),
                rcopy(bsnd.at[1, group_of(g)], blse.at[1, group_of(g)], bs.at[5, g], br.at[5, g], left)]

    def landed(copies):
        for cp in copies:
            cp.wait_recv()

    def b_early(i):
        return [rcopy(oreg(cr, i, 1), breg(0, i, 1), bs.at[0, i], br.at[0, i], right),
                rcopy(oreg(cl, i, 0), breg(1, i, 0), bs.at[1, i], br.at[1, i], left)]

    def b_late(i):
        return [rcopy(oreg(cr, i, 0), breg(0, i, 0), bs.at[2, i], br.at[2, i], right),
                rcopy(oreg(cl, i, 1), breg(1, i, 1), bs.at[3, i], br.at[3, i], left)]

    def a_merge(i):
        landed(a_send(i))
        pl.when(i % lse_group == 0)(lambda: landed(a_lse(i // lse_group)))
        pl.when(i == lse_group)(lambda: start(b_lse(0)))
        pl.when(i > 0)(lambda: start(b_late(i - 1)))
        w, fresh = [], []
        for side, cc in ((0, cr), (1, cl)):
            total, both = merged([clse[2 * i + side, pl.ds(cc, 1)], alse[side, i]])
            fresh.append(total)
            w += both
        bsnd[0, i] = jnp.concatenate([fresh[0], clse[2 * i + 1, pl.ds(cr, 1)]], axis=0)
        bsnd[1, i] = jnp.concatenate([clse[2 * i, pl.ds(cl, 1)], fresh[1]], axis=0)
        w = columns(w)
        for side, cc in ((0, cr), (1, cl)):
            for j in range(half):
                b, span = i * GO + side * half + j, slice(j * rows, (j + 1) * rows)
                x = o_all[k, cc, b].astype(jnp.float32) * w[span, 2 * side:2 * side + 1]
                y = abuf[side, i * half + j].astype(jnp.float32) * w[span, 2 * side + 1:2 * side + 2]
                o_all[k, cc, b] = (x + y).astype(jnp.bfloat16)

    def final_merge(i):
        late = b_late(i)
        landed(b_early(i))
        pl.when(i % lse_group == 0)(lambda: landed(b_lse(i // lse_group)))
        own = jnp.concatenate([clse[2 * i + h, pl.ds(c, 1)] for h in range(2)], axis=0)
        w = columns(merged([own, blse[0, i], blse[1, i]])[1])
        for h in range(2):
            late[h].wait_recv()
            for j in range(half):
                b, span = i * GO + h * half + j, slice(j * rows, (j + 1) * rows)
                x = o_all[k, c, b].astype(jnp.float32) * w[span, h:h + 1]
                x += bbuf[0, b].astype(jnp.float32) * w[span, 2 + h:3 + h]
                x += bbuf[1, b].astype(jnp.float32) * w[span, 4 + h:5 + h]
                out_ref[b] = x.astype(jnp.bfloat16)
        sent(late)

    def sent(copies):
        for cp in copies:
            cp.wait_send()

    def ring_start(lo, hi):
        lax.fori_loop(lo, hi, lambda i, carry: (start(a_send(i) + b_early(i)), carry)[1], 0)

    q_ready(0)
    pl.semaphore_wait(barrier, 3)
    for j in range(AHEAD):
        start(q_own(j))
    q_load(1)
    lengths.start()
    for b in range(KV_SLOTS):
        kv_copy(b).start()
    q_ready(1)
    lengths.wait()

    def step(j, carry):
        @pl.when(j < n_q)
        def _():
            q_arrival(0, j).wait_recv()
            q_arrival(1, j).wait_recv()
            for cp in q_relay(j):
                cp.start()

        @pl.when(j + AHEAD < n_q)
        def _():
            for cp in q_own(j + AHEAD):
                cp.start()

        @pl.when((j >= 1) & (j <= n_q))
        def _():
            q_arrival(3, j - 1).wait_recv()
            q_arrival(4, j - 1).wait_recv()
            for cp in q_far(j - 1):
                cp.start()

        for at, op in enumerate((lambda: start(a_send(0)), lambda: start(b_early(0)), lambda: ring_start(1, 2), lambda: (ring_start(2, n_o // 2), start(a_lse(0))),
                                 lambda: ring_start(n_o // 2, n_o - 2), lambda: ring_start(n_o - 2, n_o - 1))):
            pl.when(j == n_q - 4 + at)(functools.partial(lambda f: (f(), None)[1], op))

        @pl.when((j >= 4) & (j % 2 == 0))
        def _():
            start(d_send(j // 2 - 2))

        @pl.when(j >= 2)
        def _():
            s = j - 2
            for kind in (2, 5, 6, 7, 8):
                q_arrival(kind, s).wait_recv()
            lax.fori_loop(0, GQ // UNROLL, lambda n, cc: (attend(s * GQ + n * UNROLL), cc)[1], 0)

            @pl.when((s % 2 == 0) & (s > 0))
            def _():
                d_merge(s // 2 - 1)

        return carry

    def each(lo, hi, op):
        lax.fori_loop(lo, hi, lambda i, carry: (op(i), carry)[1], 0)

    each(0, n_q + 2, lambda j: step(j, 0))
    each(0, n_q // 2, lambda j: sent(q_own(j) + q_relay(j) + q_far(j)))
    start(d_send(n_o - 1))
    d_merge(n_o - 1)
    each(n_q // 2, n_q, lambda j: sent(q_own(j) + q_relay(j) + q_far(j)))
    ring_start(n_o - 1, n_o)
    start(a_lse(1))
    each(0, n_o, a_merge)
    each(0, n_o, lambda i: sent(d_send(i)))
    start(b_lse(1) + b_late(n_o - 1))
    each(0, n_o, lambda i: sent(a_send(i) + b_early(i)))
    each(0, n_o, final_merge)
    each(0, 2, lambda g: sent(a_lse(g) + b_lse(g)))


def solution(mesh):
    group = mesh.shape['dcp']
    chips = group // CORES

    def local_step(q_blk, kv_blk, len_blk):
        batch, toks, heads, width = q_blk.shape
        npos = kv_blk.shape[1] * kv_blk.shape[2] * kv_blk.shape[3]
        rows, lanes = toks * heads, GO // 2 * toks * heads
        n_q, n_o = batch // GQ, batch // GO
        bf16, f32, dma = jnp.bfloat16, jnp.float32, pltpu.SemaphoreType.DMA
        any_space = pl.BlockSpec(memory_space=pl.ANY)
        out = pl.pallas_call(
            functools.partial(_kernel, (batch, toks, heads, npos, group)),
            out_shape=pltpu.VMEM((batch, rows, LATENT), bf16),
            in_specs=[any_space, any_space, any_space],
            out_specs=pl.BlockSpec(memory_space=pltpu.VMEM),
            scratch_shapes=[
                pltpu.SMEM((batch,), jnp.int32),
                pltpu.VMEM((CORES, chips, batch, heads, toks * width), bf16),
                pltpu.VMEM((batch, toks, heads, ROPE), bf16),
                pltpu.VMEM((KV_SLOTS, npos, width), bf16),
                pltpu.VMEM((CORES, chips, batch, rows, LATENT), bf16),
                pltpu.VMEM((chips, batch, rows, LATENT), bf16),
                pltpu.VMEM((2, batch // 2, rows, LATENT), bf16),
                pltpu.VMEM((2, batch, rows, LATENT), bf16),
                pltpu.VMEM((CORES, 2 * n_o, chips, lanes), f32),
                pltpu.VMEM((2 * n_o, chips, lanes), f32),
                pltpu.VMEM((2 * n_o, chips, lanes), f32),
                pltpu.VMEM((2, n_o, 1, lanes), f32),
                pltpu.VMEM((2, n_o, 1, lanes), f32),
                pltpu.VMEM((2, n_o, 2, lanes), f32),
                pltpu.VMEM((2, n_o, 2, lanes), f32),
                dma((2, toks + 1)), dma, dma((KV_SLOTS,)),
                dma((9, n_q)), dma((9, n_q)),
                dma((2, n_o)), dma((2, n_o)),
                dma((4, n_o)), dma((4, n_o)),
                dma((6, n_o)), dma((6, n_o)),
            ],
            compiler_params=pltpu.CompilerParams(collective_id=0, has_side_effects=True, vmem_limit_bytes=63_000_000),
            name='mla_ring',
        )(q_blk, kv_blk.reshape(batch, npos, width), len_blk)
        return out.reshape(batch, toks, heads, LATENT)

    return jax.shard_map(local_step, mesh=mesh, in_specs=(P('dp', None, 'dcp', None), P('dp', None, 'dcp', None, None), P('dp')),
                         out_specs=P('dp', None, 'dcp', None), check_vma=False)
```

```python
import functools
import math

import jax
import jax.numpy as jnp
from jax import lax
from jax.experimental import pallas as pl
from jax.experimental.pallas import tpu as pltpu
from jax.sharding import PartitionSpec as P

LATENT = 512
ROPE = 64
NOPE = 128
PAGE = 64
CORES = 2
SCALE2 = (NOPE + ROPE) ** -0.5 * math.log2(math.e)

GQ = 4
GO = 8
KV_SLOTS = 4
UNROLL = 2
AHEAD = 4


def _kernel(sizes, q_hbm, kv_hbm, len_hbm, out_ref,
            len_ref, qall, rope_in, kvb, o_all, prx, abuf, bbuf,
            lse_all, plse, clse, asnd, alse, bsnd, blse,
            load_sem, len_sem, kv_sem, qs, qr, ds, dr, as_, ar, bs, br):
    batch, toks, heads, npos, group = sizes
    chips = group // CORES
    rows = toks * heads
    half = GO // 2
    n_q, n_o = batch // GQ, batch // GO
    lse_group = n_o // 2
    me = lax.axis_index('dcp')
    c, k = me // CORES, me % CORES
    ok = 1 - k
    cr, cl, cf = (c + 1) % chips, (c + chips - 1) % chips, (c + 2) % chips
    right, left, partner = cr * CORES + k, cl * CORES + k, c * CORES + ok

    barrier = pltpu.get_barrier_semaphore()
    for other in (right, left, partner):
        pl.semaphore_signal(barrier, inc=1, device_id={'dcp': other}, device_id_type=pl.DeviceIdType.MESH)

    def rcopy(src, dst, send, recv, dev):
        return pltpu.make_async_remote_copy(src_ref=src, dst_ref=dst, send_sem=send, recv_sem=recv,
                                            device_id={'dcp': dev}, device_id_type=pl.DeviceIdType.MESH)

    spans = ((0, AHEAD * GQ), (AHEAD * GQ, batch))

    def q_loads(n):
        span = slice(*spans[n])
        lat = [pltpu.make_async_copy(q_hbm.at[span, t, :, 0:LATENT], qall.at[k, c, span, :, t * LATENT:(t + 1) * LATENT], load_sem.at[n, t])
               for t in range(toks)]
        return lat, pltpu.make_async_copy(q_hbm.at[span, :, :, LATENT:LATENT + ROPE], rope_in.at[span], load_sem.at[n, toks])

    def q_ready(n):
        lat, rope = q_loads(n)
        span = slice(*spans[n])
        rope.wait()
        qall[k, c, span, :, toks * LATENT:] = jnp.concatenate([rope_in[span, t] for t in range(toks)], axis=-1)
        for cp in lat:
            cp.wait()

    def start(copies):
        for cp in copies:
            cp.start()

    def q_load(n):
        lat, rope = q_loads(n)
        start([rope] + lat)

    q_load(0)
    lengths = pltpu.make_async_copy(len_hbm, len_ref, len_sem)

    def kv_copy(b):
        slot = lax.rem(b, KV_SLOTS)
        return pltpu.make_async_copy(kv_hbm.at[b], kvb.at[slot], kv_sem.at[slot])

    def qreg(kk, cc, b0, n):
        return qall.at[kk, cc, pl.ds(b0, n)]

    def q_own(j):
        r = qreg(k, c, j * GQ, GQ)
        return [rcopy(r, r, qs.at[0, j], qr.at[0, j], right), rcopy(r, r, qs.at[1, j], qr.at[1, j], left),
                rcopy(r, r, qs.at[2, j], qr.at[2, j], partner)]

    def q_relay(j):
        lr, rr = qreg(k, cl, j * GQ, GQ), qreg(k, cr, j * GQ, GQ)
        lh, rh = qreg(k, cl, j * GQ, GQ // 2), qreg(k, cr, j * GQ + GQ // 2, GQ // 2)
        return [rcopy(lh, lh, qs.at[3, j], qr.at[3, j], right), rcopy(rh, rh, qs.at[4, j], qr.at[4, j], left),
                rcopy(lr, lr, qs.at[5, j], qr.at[5, j], partner), rcopy(rr, rr, qs.at[6, j], qr.at[6, j], partner)]

    def q_far(j):
        f0, f1 = qreg(k, cf, j * GQ, GQ // 2), qreg(k, cf, j * GQ + GQ // 2, GQ // 2)
        return [rcopy(f0, f0, qs.at[7, j], qr.at[7, j], partner), rcopy(f1, f1, qs.at[8, j], qr.at[8, j], partner)]

    def q_arrival(kind, j):
        full, h0, h1 = (j * GQ, GQ), (j * GQ, GQ // 2), (j * GQ + GQ // 2, GQ // 2)
        kk, cc, span = [(k, cl, full), (k, cr, full), (ok, c, full), (k, cf, h0), (k, cf, h1),
                        (ok, cl, full), (ok, cr, full), (ok, cf, h0), (ok, cf, h1)][kind]
        r = qreg(kk, cc, *span)
        return rcopy(r, r, qs.at[kind, j], qr.at[kind, j], partner)

    row_tok = (lax.broadcasted_iota(jnp.int32, (CORES * chips * rows, 1), 0) // heads) % toks
    key = lax.broadcasted_iota(jnp.int32, (1, npos), 1)
    pos = ((key // PAGE) * group + me) * PAGE + key % PAGE
    lanes = half * rows
    shift = lax.broadcasted_iota(jnp.int32, (chips * rows, lanes), 1) - lax.broadcasted_iota(jnp.int32, (chips * rows, lanes), 0) % rows
    lane_seq = lax.broadcasted_iota(jnp.int32, (chips, lanes), 1) // rows

    def scores(b):
        slot = lax.rem(b, KV_SLOTS)
        q = qall[:, :, b].reshape(CORES * chips, heads, toks * (LATENT + ROPE))
        lat = jnp.stack([q[:, :, t * LATENT:(t + 1) * LATENT] for t in range(toks)], axis=1).reshape(-1, LATENT)
        rope0 = toks * LATENT
        rope = jnp.stack([q[:, :, rope0 + t * ROPE:rope0 + (t + 1) * ROPE] for t in range(toks)], axis=1).reshape(-1, ROPE)
        q_rows = jnp.concatenate([lat, rope], axis=-1)
        return lax.dot_general(q_rows, kvb[slot], (((1,), (1,)), ((), ())), preferred_element_type=jnp.float32)

    def weights(b, s):
        s = jnp.where(pos <= len_ref[b] - toks + row_tok, s, -jnp.inf)
        m = jnp.max(s, axis=-1, keepdims=True)
        p = jnp.exp2((s - m) * SCALE2)
        return m, jnp.sum(p, axis=-1, keepdims=True), p.astype(jnp.bfloat16)

    def output(b, m, l, p):
        slot = lax.rem(b, KV_SLOTS)
        o = jnp.dot(p, kvb[slot, :, 0:LATENT], preferred_element_type=jnp.float32)
        o = (o * (1.0 / l)).astype(jnp.bfloat16)
        o_all[:, :, b] = o.reshape(CORES, chips, rows, LATENT)
        lse = m * SCALE2 + jnp.log2(l)
        place, in_half = b // half, b % half
        for kk in range(CORES):
            col = lse[kk * chips * rows:(kk + 1) * chips * rows]
            spread = jnp.where(shift == in_half * rows, col, 0.0).reshape(chips, rows, lanes)
            lse_all[kk, place] = jnp.where(lane_seq == in_half, jnp.sum(spread, axis=1), lse_all[kk, place])

    def attend(b0):
        bs_ = [b0 + u for u in range(UNROLL)]
        for b in bs_:
            kv_copy(b).wait()
        s = scores(bs_[0])
        for b in bs_:
            following = scores(b + 1) if b is not bs_[-1] else None
            output(b, *weights(b, s))
            s = following
        for b in bs_:
            @pl.when(b + KV_SLOTS < batch)
            def _():
                kv_copy(b + KV_SLOTS).start()

    def seqs(i, n=GO):
        return pl.ds(pl.multiple_of(i * n, n), n)

    def halves(i):
        return pl.ds(pl.multiple_of(2 * i, 2), 2)

    def columns(rows_):
        n = sum(r.shape[0] for r in rows_)
        return jnp.transpose(jnp.concatenate(rows_ + [jnp.zeros((8 - n, lanes), jnp.float32)] if n < 8 else rows_, axis=0))

    def merged(parts):
        top = functools.reduce(jnp.maximum, parts)
        total = top + jnp.log2(sum(jnp.exp2(x - top) for x in parts))
        return total, [jnp.exp2(x - total) for x in parts]

    def d_send(i):
        return [rcopy(o_all.at[ok, :, seqs(i)], prx.at[:, seqs(i)], ds.at[0, i], dr.at[0, i], partner),
                rcopy(lse_all.at[ok, halves(i)], plse.at[halves(i)], ds.at[1, i], dr.at[1, i], partner)]

    def d_merge(i):
        for cp in d_send(i):
            cp.wait_recv()
        w = []
        for h in range(2):
            total, (wa, wb) = merged([lse_all[k, 2 * i + h], plse[2 * i + h]])
            clse[2 * i + h] = total
            asnd[h, i] = clse[2 * i + h, pl.ds(cf, 1)]
            w.append(columns([wa, wb]))
        for j in range(GO):
            h, span = j // half, slice(j % half * rows, (j % half + 1) * rows)
            for cc in range(chips):
                x = o_all[k, cc, i * GO + j].astype(jnp.float32) * w[h][span, cc:cc + 1]
                y = prx[cc, i * GO + j].astype(jnp.float32) * w[h][span, chips + cc:chips + cc + 1]
                o_all[k, cc, i * GO + j] = (x + y).astype(jnp.bfloat16)

    def oreg(cc, i, part):
        if part is None:
            return o_all.at[k, cc, seqs(i)]
        return o_all.at[k, cc, pl.ds(i * GO + part * half, half)]

    def breg(side, i, part):
        return bbuf.at[side, pl.ds(i * GO + part * half, half)]

    def a_send(i):
        return [rcopy(oreg(cf, i, 0), abuf.at[0, pl.ds(i * half, half)], as_.at[0, i], ar.at[0, i], right),
                rcopy(oreg(cf, i, 1), abuf.at[1, pl.ds(i * half, half)], as_.at[1, i], ar.at[1, i], left)]

    def group_of(g):
        return pl.ds(g * lse_group, lse_group)

    def a_lse(g):
        return [rcopy(asnd.at[0, group_of(g)], alse.at[0, group_of(g)], as_.at[2, g], ar.at[2, g], right),
                rcopy(asnd.at[1, group_of(g)], alse.at[1, group_of(g)], as_.at[3, g], ar.at[3, g], left)]

    def b_lse(g):
        return [rcopy(bsnd.at[0, group_of(g)], blse.at[0, group_of(g)], bs.at[4, g], br.at[4, g], right),
                rcopy(bsnd.at[1, group_of(g)], blse.at[1, group_of(g)], bs.at[5, g], br.at[5, g], left)]

    def landed(copies):
        for cp in copies:
            cp.wait_recv()

    def b_early(i):
        return [rcopy(oreg(cr, i, 1), breg(0, i, 1), bs.at[0, i], br.at[0, i], right),
                rcopy(oreg(cl, i, 0), breg(1, i, 0), bs.at[1, i], br.at[1, i], left)]

    def b_late(i):
        return [rcopy(oreg(cr, i, 0), breg(0, i, 0), bs.at[2, i], br.at[2, i], right),
                rcopy(oreg(cl, i, 1), breg(1, i, 1), bs.at[3, i], br.at[3, i], left)]

    def a_merge(i):
        landed(a_send(i))
        pl.when(i % lse_group == 0)(lambda: landed(a_lse(i // lse_group)))
        pl.when(i == lse_group)(lambda: start(b_lse(0)))
        pl.when(i > 0)(lambda: start(b_late(i - 1)))
        w, fresh = [], []
        for side, cc in ((0, cr), (1, cl)):
            total, both = merged([clse[2 * i + side, pl.ds(cc, 1)], alse[side, i]])
            fresh.append(total)
            w += both
        bsnd[0, i] = jnp.concatenate([fresh[0], clse[2 * i + 1, pl.ds(cr, 1)]], axis=0)
        bsnd[1, i] = jnp.concatenate([clse[2 * i, pl.ds(cl, 1)], fresh[1]], axis=0)
        w = columns(w)
        for side, cc in ((0, cr), (1, cl)):
            for j in range(half):
                b, span = i * GO + side * half + j, slice(j * rows, (j + 1) * rows)
                x = o_all[k, cc, b].astype(jnp.float32) * w[span, 2 * side:2 * side + 1]
                y = abuf[side, i * half + j].astype(jnp.float32) * w[span, 2 * side + 1:2 * side + 2]
                o_all[k, cc, b] = (x + y).astype(jnp.bfloat16)

    def final_merge(i):
        late = b_late(i)
        landed(b_early(i))
        pl.when(i % lse_group == 0)(lambda: landed(b_lse(i // lse_group)))
        own = jnp.concatenate([clse[2 * i + h, pl.ds(c, 1)] for h in range(2)], axis=0)
        w = columns(merged([own, blse[0, i], blse[1, i]])[1])
        for h in range(2):
            late[h].wait_recv()
            for j in range(half):
                b, span = i * GO + h * half + j, slice(j * rows, (j + 1) * rows)
                x = o_all[k, c, b].astype(jnp.float32) * w[span, h:h + 1]
                x += bbuf[0, b].astype(jnp.float32) * w[span, 2 + h:3 + h]
                x += bbuf[1, b].astype(jnp.float32) * w[span, 4 + h:5 + h]
                out_ref[b] = x.astype(jnp.bfloat16)
        sent(late)

    def sent(copies):
        for cp in copies:
            cp.wait_send()

    def ring_start(lo, hi):
        lax.fori_loop(lo, hi, lambda i, carry: (start(a_send(i) + b_early(i)), carry)[1], 0)

    q_ready(0)
    pl.semaphore_wait(barrier, 3)
    for j in range(AHEAD):
        start(q_own(j))
    q_load(1)
    lengths.start()
    for b in range(KV_SLOTS):
        kv_copy(b).start()
    q_ready(1)
    lengths.wait()

    def step(j, carry):
        @pl.when(j < n_q)
        def _():
            q_arrival(0, j).wait_recv()
            q_arrival(1, j).wait_recv()
            for cp in q_relay(j):
                cp.start()

        @pl.when(j + AHEAD < n_q)
        def _():
            for cp in q_own(j + AHEAD):
                cp.start()

        @pl.when((j >= 1) & (j <= n_q))
        def _():
            q_arrival(3, j - 1).wait_recv()
            q_arrival(4, j - 1).wait_recv()
            for cp in q_far(j - 1):
                cp.start()

        for at, op in enumerate((lambda: start(a_send(0)), lambda: start(b_early(0)), lambda: ring_start(1, 2), lambda: (ring_start(2, n_o // 2), start(a_lse(0))),
                                 lambda: ring_start(n_o // 2, n_o - 2), lambda: ring_start(n_o - 2, n_o - 1))):
            pl.when(j == n_q - 4 + at)(functools.partial(lambda f: (f(), None)[1], op))

        @pl.when((j >= 4) & (j % 2 == 0))
        def _():
            start(d_send(j // 2 - 2))

        @pl.when(j >= 2)
        def _():
            s = j - 2
            for kind in (2, 5, 6, 7, 8):
                q_arrival(kind, s).wait_recv()
            lax.fori_loop(0, GQ // UNROLL, lambda n, cc: (attend(s * GQ + n * UNROLL), cc)[1], 0)

            @pl.when((s % 2 == 0) & (s > 0))
            def _():
                d_merge(s // 2 - 1)

        return carry

    def each(lo, hi, op):
        lax.fori_loop(lo, hi, lambda i, carry: (op(i), carry)[1], 0)

    each(0, n_q + 2, lambda j: step(j, 0))
    each(0, n_q // 2, lambda j: sent(q_own(j) + q_relay(j) + q_far(j)))
    start(d_send(n_o - 1))
    d_merge(n_o - 1)
    each(n_q // 2, n_q, lambda j: sent(q_own(j) + q_relay(j) + q_far(j)))
    ring_start(n_o - 1, n_o)
    start(a_lse(1))
    each(0, n_o, a_merge)
    each(0, n_o, lambda i: sent(d_send(i)))
    start(b_lse(1) + b_late(n_o - 1))
    each(0, n_o, lambda i: sent(a_send(i) + b_early(i)))
    each(0, n_o, final_merge)
    each(0, 2, lambda g: sent(a_lse(g) + b_lse(g)))


def solution(mesh):
    group = mesh.shape['dcp']
    chips = group // CORES

    def local_step(q_blk, kv_blk, len_blk):
        batch, toks, heads, width = q_blk.shape
        npos = kv_blk.shape[1] * kv_blk.shape[2] * kv_blk.shape[3]
        rows, lanes = toks * heads, GO // 2 * toks * heads
        n_q, n_o = batch // GQ, batch // GO
        bf16, f32, dma = jnp.bfloat16, jnp.float32, pltpu.SemaphoreType.DMA
        any_space = pl.BlockSpec(memory_space=pl.ANY)
        out = pl.pallas_call(
            functools.partial(_kernel, (batch, toks, heads, npos, group)),
            out_shape=pltpu.VMEM((batch, rows, LATENT), bf16),
            in_specs=[any_space, any_space, any_space],
            out_specs=pl.BlockSpec(memory_space=pltpu.VMEM),
            scratch_shapes=[
                pltpu.SMEM((batch,), jnp.int32),
                pltpu.VMEM((CORES, chips, batch, heads, toks * width), bf16),
                pltpu.VMEM((batch, toks, heads, ROPE), bf16),
                pltpu.VMEM((KV_SLOTS, npos, width), bf16),
                pltpu.VMEM((CORES, chips, batch, rows, LATENT), bf16),
                pltpu.VMEM((chips, batch, rows, LATENT), bf16),
                pltpu.VMEM((2, batch // 2, rows, LATENT), bf16),
                pltpu.VMEM((2, batch, rows, LATENT), bf16),
                pltpu.VMEM((CORES, 2 * n_o, chips, lanes), f32),
                pltpu.VMEM((2 * n_o, chips, lanes), f32),
                pltpu.VMEM((2 * n_o, chips, lanes), f32),
                pltpu.VMEM((2, n_o, 1, lanes), f32),
                pltpu.VMEM((2, n_o, 1, lanes), f32),
                pltpu.VMEM((2, n_o, 2, lanes), f32),
                pltpu.VMEM((2, n_o, 2, lanes), f32),
                dma((2, toks + 1)), dma, dma((KV_SLOTS,)),
                dma((9, n_q)), dma((9, n_q)),
                dma((2, n_o)), dma((2, n_o)),
                dma((4, n_o)), dma((4, n_o)),
                dma((6, n_o)), dma((6, n_o)),
            ],
            compiler_params=pltpu.CompilerParams(collective_id=0, has_side_effects=True, vmem_limit_bytes=63_000_000),
            name='mla_ring',
        )(q_blk, kv_blk.reshape(batch, npos, width), len_blk)
        return out.reshape(batch, toks, heads, LATENT)

    return jax.shard_map(local_step, mesh=mesh, in_specs=(P('dp', None, 'dcp', None), P('dp', None, 'dcp', None, None), P('dp')),
                         out_specs=P('dp', None, 'dcp', None), check_vma=False)
```
